32 devices in a mesh: grp: 2 (over x), lon: 4 (over y, core), lat: 4 (over z).
Axes of the slice: x: 2, y: 2, z: 4, core: 2. Of those that a mesh axis runs over, the one named last changes fastest.
Arguments:
- fields: bfloat16 [6, 2, 48, 48, 512], P('grp', None, 'lat', 'lon'), may hold values from -6 to 6
- surface_mask: int32 [2, 48, 48], P(None, 'lat', 'lon'), may hold values 0 or 1
- w_qkv: bfloat16 [512, 1536], replicated, may hold values from -0.25 to 0.25
- w_out: bfloat16 [512, 512], replicated, may hold values from -0.25 to 0.25
- logit_scale: float32 [8], replicated, may hold values from 2 to 12
- mask_bias: float32 [8], replicated, may hold values from -2 to 2
- w_up: bfloat16 [512, 2048], replicated, may hold values from -0.25 to 0.25
- w_down: bfloat16 [2048, 512], replicated, may hold values from -0.125 to 0.125
Outputs:
- joined: bfloat16 [6, 2, 48, 48, 512], P('grp', None, 'lat', 'lon')
The draws below stay inside these ranges and needn't reach their ends.
All inputs are finite; a program needn't handle non-finite values. No bound on the sum of `surface_mask` on one device may be relied on, other than what follows from the above.
Results may differ from the reference program's by a relative error of at most 0.006.
Values may be sent and summed in bfloat16 or wider, within the bound.
A program may use at most 128 MiB of HBM per device.

```python
import math
import jax
import jax.numpy as jnp
from jax import lax

G = 6
LEV = 2
C = 512
HEADS = 8
HIDDEN_SIZE = 2048
WLAT = 6
WLON = 12
SH_LAT = 3
SH_LON = 6
NLAT = 48
NLON = 48


def plant(array, rng, least, largest):
    index_at = [jax.random.randint(jax.random.fold_in(rng, axis), (), 0, length) for axis, length in enumerate(array.shape)]
    main_axis = array.shape.index(max(array.shape))
    neighbour = index_at[:main_axis] + [(index_at[main_axis] + 1) % array.shape[main_axis]] + index_at[main_axis + 1:]
    return array.at[tuple(index_at)].set(least).at[tuple(neighbour)].set(largest)


def level_of(key, extent, pieces, least, largest):
    loudness = 1.0
    for position, shards_of in pieces:
        heights = jax.random.uniform(jax.random.fold_in(jax.random.fold_in(key, 6), position), (shards_of,), jnp.float32, least / len(pieces), largest / len(pieces))
        loudness = loudness * jnp.repeat(jnp.exp(heights), extent[position] // shards_of).reshape((-1,) + (1,) * (len(extent) - 1 - position))
    return loudness


def bell_draw(key, shape, deviation, limit, split=(), kind=jnp.bfloat16):
    array = jax.random.normal(key, shape, jnp.float32) * deviation
    if len(split) > 0:
        array = level_of(key, shape, split, -0.22, 0.18) * array
    return jnp.clip(array, min=-limit, max=limit).astype(kind)


def setup_inputs(seed: int = 0) -> dict:
    seeds = jax.random.split(jax.random.key(seed), 9)
    fields = bell_draw(seeds[0], (G, LEV, NLAT, NLON, C), 1.0, 6.0, ((0, 2), (2, 4), (3, 4)))
    surface_mask = plant((jax.random.randint(seeds[1], (LEV, NLAT, NLON), 0, 2) < 1).astype(jnp.int32), jax.random.fold_in(seeds[1], 1), 0, 1)
    w_qkv = bell_draw(seeds[2], (C, 3 * C), C ** -0.5, 0.25)
    w_out = bell_draw(seeds[3], (C, C), C ** -0.5, 0.25)
    logit_scale = jnp.clip(jnp.exp(jax.random.uniform(seeds[4], (HEADS,), jnp.float32, math.log(2.0), math.log(12.0))), 2.0, 12.0)
    mask_bias = jnp.clip(jax.random.uniform(seeds[5], (HEADS,), jnp.float32, -2.0, 2.0), -2.0, 2.0)
    w_up = bell_draw(seeds[6], (C, HIDDEN_SIZE), C ** -0.5, 0.25)
    w_down = bell_draw(seeds[7], (HIDDEN_SIZE, C), HIDDEN_SIZE ** -0.5, 0.125)
    return {"fields": fields, "surface_mask": surface_mask, "w_qkv": w_qkv, "w_out": w_out, "logit_scale": logit_scale, "mask_bias": mask_bias, "w_up": w_up, "w_down": w_down}


def layer_norm(values):
    centred = values - lax.optimization_barrier(jnp.mean(values, -1, keepdims=True))
    return centred * lax.rsqrt(lax.optimization_barrier(jnp.mean(centred * centred, -1, keepdims=True)) + 1e-05)

def unit_heads(mixed_part, head_count):
    shaped = mixed_part.reshape(mixed_part.shape[0], head_count, -1)
    scaled = shaped * lax.rsqrt(lax.optimization_barrier(jnp.mean(shaped * shaped, -1, keepdims=True)) + 1e-06)
    return scaled.reshape(mixed_part.shape).astype(jnp.bfloat16)

def windowed(tensor, nlat, nlon):
    lead = tensor.shape[:2]
    rest = tensor.shape[4:]
    shaped = tensor.reshape(lead + (nlat // WLAT, WLAT, nlon // WLON, WLON) + rest)
    order = (2, 4, 0, 1, 3, 5) + tuple(range(6, 6 + len(rest)))
    moved = jnp.transpose(shaped, order)
    return moved.reshape((nlat // WLAT * (nlon // WLON), lead[0] * lead[1] * WLAT * WLON) + rest)

def attend_window(window_args, scale, head_count):
    query_win, key_win, value_win, bias_win, region_win = window_args
    tokens, model_width = query_win.shape
    head_size = model_width // head_count
    query_heads = query_win.astype(jnp.float32).reshape(tokens, head_count, head_size)
    key_heads = key_win.astype(jnp.float32).reshape(tokens, head_count, head_size)
    value_heads = value_win.astype(jnp.float32).reshape(tokens, head_count, head_size)
    scores = jnp.einsum('qhd,khd->hqk', query_heads, key_heads)
    scores = scores * (scale / head_size)[:, None, None] + bias_win[:, None, :]
    same_region = region_win[:, None] == region_win[None, :]
    weights = jnp.where(same_region[None], jnp.exp(scores), 0.0).astype(jnp.bfloat16)
    weights = lax.optimization_barrier(weights).astype(jnp.float32)
    totals = lax.optimization_barrier(jnp.sum(weights, -1))
    weighted = jnp.einsum('hqk,khd->qhd', weights, value_heads)
    ratio = weighted / jnp.transpose(totals)[:, :, None]
    return ratio.astype(jnp.bfloat16).reshape(tokens, model_width)

def reference(fields, surface_mask, w_qkv, w_out, logit_scale, mask_bias, w_up, w_down):
    groups, levels, nlat, nlon, model_width = fields.shape
    head_count = logit_scale.shape[0]
    rolled = jnp.roll(fields, (-SH_LAT, -SH_LON), axis=(2, 3))
    marks = jnp.roll(surface_mask, (-SH_LAT, -SH_LON), axis=(1, 2)).astype(jnp.float32)
    normed = layer_norm(rolled.astype(jnp.float32)).astype(jnp.bfloat16)
    mixed = jnp.dot(normed.reshape(-1, model_width), w_qkv, preferred_element_type=jnp.float32)
    grid_shape = (groups, levels, nlat, nlon, model_width)
    queries = unit_heads(mixed[:, :model_width], head_count).reshape(grid_shape)
    key_part = unit_heads(mixed[:, model_width:2 * model_width], head_count).reshape(grid_shape)
    value_part = mixed[:, 2 * model_width:].astype(jnp.bfloat16).reshape(grid_shape)
    window_count = nlat // WLAT * (nlon // WLON)
    key_bias = mask_bias[:, None, None, None] * marks[None]
    key_bias = key_bias.reshape(head_count, levels, nlat // WLAT, WLAT, nlon // WLON, WLON)
    key_bias = jnp.transpose(key_bias, (2, 4, 0, 1, 3, 5)).reshape(window_count, head_count, -1)
    key_bias = jnp.tile(key_bias, (1, 1, groups))
    row_ids = jnp.arange(nlat, dtype=jnp.int32)
    flag_rows = (row_ids >= nlat - SH_LAT).astype(jnp.int32)
    flag_grid = jnp.broadcast_to(flag_rows[None, None, :, None], (1, levels, nlat, nlon))
    region_win = jnp.tile(windowed(flag_grid, nlat, nlon), (1, groups))

    def attend_block(window_args):
        return attend_window(window_args, logit_scale, head_count)
    attended = lax.map(attend_block, (windowed(queries, nlat, nlon), windowed(key_part, nlat, nlon), windowed(value_part, nlat, nlon), key_bias, region_win))
    attended = attended.reshape(nlat // WLAT, nlon // WLON, groups, levels, WLAT, WLON, model_width)
    attended = jnp.transpose(attended, (2, 3, 0, 4, 1, 5, 6)).reshape(grid_shape)
    projected = jnp.dot(attended.reshape(-1, model_width), w_out, preferred_element_type=jnp.float32)
    projected = projected.astype(jnp.bfloat16).reshape(grid_shape)
    unrolled = jnp.roll(projected, (SH_LAT, SH_LON), axis=(2, 3))
    residual = (fields.astype(jnp.float32) + unrolled.astype(jnp.float32)).astype(jnp.bfloat16)
    mlp_in = layer_norm(residual.astype(jnp.float32)).astype(jnp.bfloat16)
    hidden = jax.nn.gelu(jnp.dot(mlp_in.reshape(-1, model_width), w_up, preferred_element_type=jnp.float32), approximate=True).astype(jnp.bfloat16)
    update = jnp.dot(hidden, w_down, preferred_element_type=jnp.float32).reshape(grid_shape)
    return (residual.astype(jnp.float32) + update).astype(jnp.bfloat16)
```

```python
import functools
import math

import jax
import jax.numpy as jnp
from jax import lax
from jax.experimental import pallas as pl
from jax.experimental.pallas import tpu as pltpu
from jax.sharding import PartitionSpec as P

SH_LAT = 3
SH_LON = 6
LOG2E = math.log2(math.e)
FAR = -30000.0
MESH = pl.DeviceIdType.MESH
BF16 = jnp.bfloat16
F32 = jnp.float32


def layer_norm(values):
    centred = values - jnp.mean(values, -1, keepdims=True)
    return centred * lax.rsqrt(jnp.mean(centred * centred, -1, keepdims=True) + 1e-05)


def iota(shape, axis):
    return lax.broadcasted_iota(jnp.int32, shape, axis)


def dot(left, right):
    return jnp.dot(left, right, preferred_element_type=F32)


def dot_t(left, right):
    return lax.dot_general(left, right, (((1,), (1,)), ((), ())), preferred_element_type=F32)


def kernel(
    real, heads,
    x_ref, qscale_ref, bias_ref, wqkv_hbm, wout_hbm, wup_hbm, wdown_hbm,
    out_ref,
    wqkv, wout, wup, wdown, win, ret, proj, att, qs, ks, vs, kx,
    wsem, send1, recv1, send2, recv2,
):
    rows, width = x_ref.shape[2:]
    pair_rows = 2 * rows
    half = 2 * pair_rows
    total = 2 * half
    pairs = heads // 2
    head_size = width // heads
    lanes = 2 * head_size

    g, a, b = lax.axis_index("grp"), lax.axis_index("lat"), lax.axis_index("lon")
    na, nb = lax.axis_size("lat"), lax.axis_size("lon")

    weights = [
        pltpu.make_async_copy(src, dst, wsem.at[i])
        for i, (src, dst) in enumerate(
            ((wqkv_hbm, wqkv), (wout_hbm, wout), (wup_hbm, wup), (wdown_hbm, wdown))
        )
    ]
    for copy in weights:
        copy.start()

    barrier = pltpu.get_barrier_semaphore()
    greeted = 0
    for d in (0, 1):
        for da in (-1, 0, 1):
            for db in (-1, 0, 1):
                if d or da or db:
                    pl.semaphore_signal(
                        barrier,
                        inc=1,
                        device_id={
                            "grp": (g + d) % 2,
                            "lat": (a + da + na) % na,
                            "lon": (b + db + nb) % nb,
                        },
                        device_id_type=MESH,
                    )
                    greeted += 1
    pl.semaphore_wait(barrier, greeted)

    def parity_to(d, cc):
        return (g + d + b + cc) % 2

    def row_of(parity, rr):
        return (1 + 2 * parity + rr) % 4

    def forward(d, cc, rr, act):
        parity = parity_to(d, cc)
        r = row_of(parity, rr)
        p = 2 * d + cc
        src = x_ref.at[r, 1 - cc]
        dst = win.at[p, rr]
        i = 2 * p + rr
        edge = rr * parity

        def local():
            return pltpu.make_async_copy(src, dst, recv1.at[i])

        def remote():
            return pltpu.make_async_remote_copy(
                src_ref=src, dst_ref=dst, send_sem=send1.at[i], recv_sem=recv1.at[i],
                device_id={
                    "grp": (g + d) % 2,
                    "lat": (a - edge + na) % na,
                    "lon": (b - cc + nb) % nb,
                },
                device_id_type=MESH,
            )

        act(d, cc, rr, parity, local, remote)

    def backward(d, cc, rr, act):
        parity = (g + b) % 2
        p = 2 * d + cc
        src = proj.at[p, rr]
        dst = ret.at[p, rr]
        i = 2 * p + rr
        edge = rr * parity

        def local():
            return pltpu.make_async_copy(src, dst, recv2.at[i])

        def remote():
            return pltpu.make_async_remote_copy(
                src_ref=src, dst_ref=dst, send_sem=send2.at[i], recv_sem=recv2.at[i],
                device_id={
                    "grp": (g + d) % 2,
                    "lat": (a + edge) % na,
                    "lon": (b + cc) % nb,
                },
                device_id_type=MESH,
            )

        act(d, cc, rr, parity, local, remote)

    def start(d, cc, rr, parity, local, remote):
        if d or cc:
            remote().start()
        elif rr == 0:
            local().start()
        else:
            pl.when(parity == 0)(lambda: local().start())
            pl.when(parity == 1)(lambda: remote().start())

    def finish(d, cc, rr, parity, local, remote):
        if d or cc:
            remote().wait_send()
        elif rr == 1:
            pl.when(parity == 1)(lambda: remote().wait_send())

    for d, cc in ((1, 0), (1, 1), (0, 1), (0, 0)):
        for rr in (1, 0):
            forward(d, cc, rr, start)

    last = jnp.where(a == na - 1, (g + b) % 2, 0)
    row_in_block = iota((pair_rows, lanes), 0) % rows
    valid = row_in_block < real
    lane = iota((pair_rows, lanes), 1)
    late = jnp.where(iota((pair_rows, lanes), 0) >= rows, last, 0)
    raw_bias = bias_ref[...]
    bias_hi = raw_bias.astype(BF16).astype(F32)
    bias_row = jnp.where(iota(raw_bias.shape, 1) % 2 == 0, bias_hi, raw_bias - bias_hi)
    far = jnp.where(
        lane == 2 * heads, FAR * late.astype(F32),
        jnp.where(lane == 2 * heads + 1, FAR * (1 - late).astype(F32), 0.0),
    )
    span = 2 * lanes
    blocks = jnp.where(
        iota((span, span), 0) // head_size == iota((span, span), 1) // head_size,
        1.0 / head_size, 0.0,
    ).astype(BF16)
    eye = jnp.where(iota((rows, lanes), 0) == iota((rows, lanes), 1), 1.0, 0.0).astype(BF16)
    ones = jnp.where(valid, 1.0, 0.0).astype(BF16)

    weights[0].wait()

    def project(p, carry):
        for rr in (0, 1):
            pltpu.make_async_copy(win.at[p, rr], win.at[p, rr], recv1.at[2 * p + rr]).wait()
        both = win[p].reshape(pair_rows, width)
        normed = layer_norm(both.astype(F32)).astype(BF16)
        here = pl.ds(p * pair_rows, pair_rows)
        for part, store in ((0, qs), (1, ks)):
            for s in range(width // span):
                lo = s * span
                mixed = dot(normed, wqkv[:, part * width + lo : part * width + lo + span])
                square = dot((mixed * mixed).astype(BF16), blocks)
                unit = mixed * lax.rsqrt(square + 1e-06)
                if part == 0:
                    unit = unit * qscale_ref[:, lo : lo + span]
                unit = unit.astype(BF16)
                store[2 * s, here] = unit[:, :lanes]
                store[2 * s + 1, here] = unit[:, lanes:]
        for s in range(width // span):
            lo = 2 * width + s * span
            mixed = dot(normed, wqkv[:, lo : lo + span])
            for k in (0, 1):
                vs[2 * s + k, here] = jnp.where(
                    valid, mixed[:, k * lanes : (k + 1) * lanes], 0.0
                ).astype(BF16)
        marks = jnp.concatenate(
            [
                dot_t(eye, jnp.broadcast_to(win[p, rr, real : real + 1, :lanes], (lanes, lanes)))
                for rr in (0, 1)
            ],
            0,
        )
        kx[here] = (marks * bias_row + far).astype(BF16)
        return carry

    lax.fori_loop(0, 4, project, 0)
    weights[1].wait()

    q_lane = iota((half, lanes), 1)
    q_late = jnp.where((iota((half, lanes), 0) // rows) % 2 == 1, last, 0)
    q_region = jnp.where(
        q_lane == 2 * heads, (1 - q_late).astype(F32),
        jnp.where(q_lane == 2 * heads + 1, q_late.astype(F32), 0.0),
    )
    low = q_lane < head_size
    ones_all = jnp.concatenate([ones] * (total // pair_rows), 0)

    for d in (1, 0):

        def attend(pair, carry):
            query = qs[pair, d * half : (d + 1) * half]
            keys = jnp.concatenate([ks[pair], kx[...]], 1)
            values = jnp.concatenate([vs[pair], ones_all], 1)
            ratios = []
            for e in (0, 1):
                chosen = jnp.where(low if e == 0 else ~low, query.astype(F32), 0.0).astype(BF16)
                extra = jnp.where(q_lane // 2 == 2 * pair + e, 1.0, q_region).astype(BF16)
                scores = dot_t(jnp.concatenate([chosen, extra], 1), keys)
                summed = dot(jnp.exp2(scores).astype(BF16), values)
                ratios.append(summed[:, :lanes] / summed[:, lanes:])
            att[:, pl.ds(pl.multiple_of(pair * lanes, lanes), lanes)] = jnp.where(
                low, ratios[0], ratios[1]
            ).astype(BF16)
            return carry

        lax.fori_loop(0, pairs, attend, 0)
        projected = dot(att[...], wout[...]).astype(BF16)
        proj[2 * d : 2 * d + 2] = projected.reshape(2, 2, rows, width)
        for cc in (1, 0):
            for rr in (1, 0):
                backward(d, cc, rr, start)

    weights[2].wait()
    weights[3].wait()

    def join(p, carry):
        for rr in (0, 1):
            pltpu.make_async_copy(ret.at[p, rr], ret.at[p, rr], recv2.at[2 * p + rr]).wait()
        d, cc = p // 2, p % 2
        parity = parity_to(d, cc)
        r0, r1 = row_of(parity, 0), row_of(parity, 1)
        own = jnp.concatenate([x_ref[r0, 1 - cc], x_ref[r1, 1 - cc]], 0)
        back = ret[p].reshape(pair_rows, width)
        residual = (own.astype(F32) + back.astype(F32)).astype(BF16).astype(F32)
        mlp_in = layer_norm(residual).astype(BF16)
        joined = residual
        hidden_size = wup.shape[1]
        piece = 512
        for s in range(hidden_size // piece):
            up = dot(mlp_in, wup[:, s * piece : (s + 1) * piece])
            inner = math.sqrt(2.0 / math.pi) * (up + 0.044715 * (up * up * up))
            hidden = (0.5 * up * (1.0 + jnp.tanh(inner))).astype(BF16)
            joined = joined + dot(hidden, wdown[s * piece : (s + 1) * piece, :])
        joined = joined.astype(BF16)
        out_ref[r0, 1 - cc] = joined[:rows]
        out_ref[r1, 1 - cc] = joined[rows:]
        return carry

    lax.fori_loop(0, 4, join, 0)

    for d in (0, 1):
        for cc in (0, 1):
            for rr in (0, 1):
                forward(d, cc, rr, finish)
                backward(d, cc, rr, finish)


def per_device(fields, surface_mask, w_qkv, w_out, logit_scale, mask_bias, w_up, w_down):
    groups, levels, nlat, nlon, width = fields.shape
    heads = logit_scale.shape[0]
    head_size = width // heads
    hidden_size = w_up.shape[1]
    tris, sides = nlat // SH_LAT, nlon // SH_LON
    real = groups * levels * SH_LAT * SH_LON
    rows = -(-(real + 1) // 16) * 16
    total = 8 * rows

    split = fields.reshape(groups, levels, tris, SH_LAT, sides, SH_LON, width)
    tokens = jnp.transpose(split, (2, 4, 0, 1, 3, 5, 6)).reshape(tris, sides, real, width)
    flags = surface_mask.reshape(levels, tris, SH_LAT, sides, SH_LON)
    flags = jnp.transpose(flags, (1, 3, 0, 2, 4)).reshape(tris, sides, 1, real // groups)
    flags = jnp.tile(flags.astype(BF16), (1, 1, 1, groups))
    flags = jnp.pad(flags, ((0, 0), (0, 0), (0, rows - real - 1), (0, width - real)))
    x = jnp.concatenate([tokens, flags], 2)

    qscale = jnp.repeat(logit_scale * (LOG2E / head_size), head_size)[None]
    bias = jnp.pad(jnp.repeat(mask_bias * LOG2E, 2), (0, 2 * head_size - 2 * heads))[None]

    vmem = pl.BlockSpec(memory_space=pltpu.VMEM)
    anywhere = pl.BlockSpec(memory_space=pl.ANY)
    joined = pl.pallas_call(
        functools.partial(kernel, real, heads),
        out_shape=jax.ShapeDtypeStruct(x.shape, BF16),
        in_specs=[vmem] * 3 + [anywhere] * 4,
        out_specs=vmem,
        scratch_shapes=[
            pltpu.VMEM(w_qkv.shape, BF16),
            pltpu.VMEM(w_out.shape, BF16),
            pltpu.VMEM(w_up.shape, BF16),
            pltpu.VMEM(w_down.shape, BF16),
            pltpu.VMEM((4, 2, rows, width), BF16),
            pltpu.VMEM((4, 2, rows, width), BF16),
            pltpu.VMEM((4, 2, rows, width), BF16),
            pltpu.VMEM((total // 2, width), BF16),
            pltpu.VMEM((heads // 2, total, 2 * head_size), BF16),
            pltpu.VMEM((heads // 2, total, 2 * head_size), BF16),
            pltpu.VMEM((heads // 2, total, 2 * head_size), BF16),
            pltpu.VMEM((total, 2 * head_size), BF16),
            pltpu.SemaphoreType.DMA((4,)),
            pltpu.SemaphoreType.DMA((8,)),
            pltpu.SemaphoreType.DMA((8,)),
            pltpu.SemaphoreType.DMA((8,)),
            pltpu.SemaphoreType.DMA((8,)),
        ],
        compiler_params=pltpu.CompilerParams(
            collective_id=0, has_side_effects=True, vmem_limit_bytes=56 * 1024 * 1024
        ),
        name="window_block",
    )(x, qscale, bias, w_qkv, w_out, w_up, w_down)

    kept = joined[:, :, :real].reshape(tris, sides, groups, levels, SH_LAT, SH_LON, width)
    return jnp.transpose(kept, (2, 3, 0, 4, 1, 5, 6)).reshape(fields.shape)


def solution(mesh):
    return jax.shard_map(
        per_device,
        mesh=mesh,
        in_specs=(
            P("grp", None, "lat", "lon", None),
            P(None, "lat", "lon"),
            P(),
            P(),
            P(),
            P(),
            P(),
            P(),
        ),
        out_specs=P("grp", None, "lat", "lon", None),
        check_vma=False,
    )
```

```python
import functools
import math

import jax
import jax.numpy as jnp
from jax import lax
from jax.experimental import pallas as pl
from jax.experimental.pallas import tpu as pltpu
from jax.sharding import PartitionSpec as P

SH_LAT = 3
SH_LON = 6
LOG2E = math.log2(math.e)
FAR = -30000.0
MESH = pl.DeviceIdType.MESH
BF16 = jnp.bfloat16
F32 = jnp.float32


def layer_norm(values):
    centred = values - jnp.mean(values, -1, keepdims=True)
    return centred * lax.rsqrt(jnp.mean(centred * centred, -1, keepdims=True) + 1e-05)


def iota(shape, axis):
    return lax.broadcasted_iota(jnp.int32, shape, axis)


def dot(left, right):
    return jnp.dot(left, right, preferred_element_type=F32)


def dot_t(left, right):
    return lax.dot_general(left, right, (((1,), (1,)), ((), ())), preferred_element_type=F32)


def kernel(
    real, heads,
    fields_hbm, flags_ref, scale_ref, bias_ref, wqkv_hbm, wout_hbm, wup_hbm, wdown_hbm,
    out_hbm,
    raw, x_ref, wqkv, wout, wup, wdown, win, ret, proj, att, qs, ks, vs, kx, acc, out_ref, outs,
    wsem, osem, send1, recv1, send2, recv2,
):
    rows, width = x_ref.shape[2:]
    groups, levels, _, cells = raw.shape[:4]
    deep = -(-cells // 16) * 16
    slabs = groups * levels * SH_LAT
    pair_rows = 2 * rows
    half = 2 * pair_rows
    total = 2 * half
    pairs = heads // 2
    head_size = width // heads
    lanes = 2 * head_size

    g, a, b = lax.axis_index("grp"), lax.axis_index("lat"), lax.axis_index("lon")
    na, nb = lax.axis_size("lat"), lax.axis_size("lon")

    barrier = pltpu.get_barrier_semaphore()
    greeted = 0
    for d in (0, 1):
        for da in (-1, 0, 1):
            for db in (-1, 0, 1):
                if d or da or db:
                    pl.semaphore_signal(
                        barrier,
                        inc=1,
                        device_id={
                            "grp": (g + d) % 2,
                            "lat": (a + da + na) % na,
                            "lon": (b + db + nb) % nb,
                        },
                        device_id_type=MESH,
                    )
                    greeted += 1
    load = pltpu.make_async_copy(fields_hbm, raw, wsem.at[4])
    load.start()
    weights = [
        pltpu.make_async_copy(src, dst, wsem.at[i])
        for i, (src, dst) in enumerate(
            ((wqkv_hbm, wqkv), (wout_hbm, wout), (wup_hbm, wup), (wdown_hbm, wdown))
        )
    ]
    for copy in weights:
        copy.start()

    def parity_to(d, cc):
        return (g + d + b + cc) % 2

    def row_of(parity, rr):
        return (1 + 2 * parity + rr) % 4

    def forward(r, c, act):
        parity, rr = (1, 1) if r == 0 else ((r - 1) // 2, (r - 1) % 2)
        cc = 1 - c
        d = (parity + g + b + cc) % 2
        p = 2 * d + cc
        src = x_ref.at[r, c]
        dst = win.at[p, rr]
        i = 2 * p + rr

        def local():
            return pltpu.make_async_copy(src, dst, recv1.at[i])

        def remote():
            return pltpu.make_async_remote_copy(
                src_ref=src, dst_ref=dst, send_sem=send1.at[i], recv_sem=recv1.at[i],
                device_id={
                    "grp": (g + d) % 2,
                    "lat": (a - 1 + na) % na if r == 0 else a,
                    "lon": (b - cc + nb) % nb,
                },
                device_id_type=MESH,
            )

        if r == 0 or cc:
            act(remote())
        else:
            pl.when(d == 1)(lambda: act(remote()))
            if act is begin:
                pl.when(d == 0)(lambda: act(local()))

    def begin(copy):
        copy.start()

    def drain(copy):
        copy.wait_send()

    def backward(d, cc, rr, act):
        parity = (g + b) % 2
        p = 2 * d + cc
        src = proj.at[p, rr]
        dst = ret.at[p, rr]
        i = 2 * p + rr
        edge = rr * parity

        def local():
            return pltpu.make_async_copy(src, dst, recv2.at[i])

        def remote():
            return pltpu.make_async_remote_copy(
                src_ref=src, dst_ref=dst, send_sem=send2.at[i], recv_sem=recv2.at[i],
                device_id={
                    "grp": (g + d) % 2,
                    "lat": (a + edge) % na,
                    "lon": (b + cc) % nb,
                },
                device_id_type=MESH,
            )

        act(d, cc, rr, parity, local, remote)

    def start(d, cc, rr, parity, local, remote):
        if d or cc:
            remote().start()
        elif rr == 0:
            local().start()
        else:
            pl.when(parity == 0)(lambda: local().start())
            pl.when(parity == 1)(lambda: remote().start())

    def finish(d, cc, rr, parity, local, remote):
        if d or cc:
            remote().wait_send()
        elif rr == 1:
            pl.when(parity == 1)(lambda: remote().wait_send())

    token = iota((2 * rows, 1), 0)
    inside = token % rows
    place = jnp.where(
        inside < real, inside // SH_LON * deep + inside % SH_LON + token // rows * SH_LON, -1
    )
    pick = jnp.where(iota((2 * rows, slabs * deep), 1) == place, 1.0, 0.0).astype(BF16)

    load.wait()
    order = (0, 3, 1, 2)
    empty = jnp.zeros((deep - cells, width), BF16)

    def sort_row(r):
        pieces = []
        for gl in range(groups * levels):
            for i in range(SH_LAT):
                pieces += [raw[gl // levels, gl % levels, SH_LAT * r + i], empty]
        sorted_rows = dot(pick, jnp.concatenate(pieces, 0)).astype(BF16)
        for c in (0, 1):
            x_ref[r, c] = sorted_rows[c * rows : (c + 1) * rows]
            x_ref[r, c, rows - 16 :, :128] = (
                sorted_rows[(c + 1) * rows - 16 : (c + 1) * rows, :128] + flags_ref[r, c]
            )

    sort_row(order[0])
    with jax.named_scope("greet"):
        pl.semaphore_wait(barrier, greeted)
    for k in range(4):
        if k < 3:
            sort_row(order[k + 1])
        for c in (0, 1):
            forward(order[k], c, begin)

    last = jnp.where(a == na - 1, (g + b) % 2, 0)
    row_in_block = iota((pair_rows, lanes), 0) % rows
    valid = row_in_block < real
    lane = iota((pair_rows, lanes), 1)
    late = jnp.where(iota((pair_rows, lanes), 0) >= rows, last, 0)
    raw_bias = jnp.zeros((1, lanes), F32)
    qscale = jnp.zeros((1, width), F32)
    for h in range(heads):
        raw_bias = jnp.where(
            iota((1, lanes), 1) // 2 == h, bias_ref[h] * LOG2E, raw_bias
        )
        qscale = jnp.where(
            iota((1, width), 1) // head_size == h, scale_ref[h] * (LOG2E / head_size), qscale
        )
    bias_hi = raw_bias.astype(BF16).astype(F32)
    bias_row = jnp.where(iota(raw_bias.shape, 1) % 2 == 0, bias_hi, raw_bias - bias_hi)
    far = jnp.where(
        lane == 2 * heads, FAR * late.astype(F32),
        jnp.where(lane == 2 * heads + 1, FAR * (1 - late).astype(F32), 0.0),
    )
    span = 2 * lanes
    blocks = jnp.where(
        iota((span, span), 0) // head_size == iota((span, span), 1) // head_size,
        1.0 / head_size, 0.0,
    ).astype(BF16)
    eye = jnp.where(iota((rows, lanes), 0) == iota((rows, lanes), 1), 1.0, 0.0).astype(BF16)
    ones = jnp.where(valid, 1.0, 0.0).astype(BF16)

    with jax.named_scope("wait_w"):
        weights[0].wait()

    def project(p, carry):
        with jax.named_scope("wait_in"):
            for rr in (0, 1):
                pltpu.make_async_copy(win.at[p, rr], win.at[p, rr], recv1.at[2 * p + rr]).wait()
        both = win[p].reshape(pair_rows, width)
        normed = layer_norm(both.astype(F32)).astype(BF16)
        here = pl.ds(p * pair_rows, pair_rows)
        for part, store in ((0, qs), (1, ks)):
            for s in range(width // span):
                lo = s * span
                mixed = dot(normed, wqkv[:, part * width + lo : part * width + lo + span])
                square = dot((mixed * mixed).astype(BF16), blocks)
                unit = mixed * lax.rsqrt(square + 1e-06)
                if part == 0:
                    unit = unit * qscale[:, lo : lo + span]
                unit = unit.astype(BF16)
                store[2 * s, here] = unit[:, :lanes]
                store[2 * s + 1, here] = unit[:, lanes:]
        for s in range(width // span):
            lo = 2 * width + s * span
            mixed = dot(normed, wqkv[:, lo : lo + span])
            for k in (0, 1):
                vs[2 * s + k, here] = jnp.where(
                    valid, mixed[:, k * lanes : (k + 1) * lanes], 0.0
                ).astype(BF16)
        marks = jnp.concatenate(
            [
                dot_t(eye, jnp.broadcast_to(win[p, rr, real : real + 1, :lanes], (lanes, lanes)))
                for rr in (0, 1)
            ],
            0,
        )
        kx[here] = (marks * bias_row + far).astype(BF16)
        return carry

    def attend(q0, nq, k0, nk, first, final):
        q_lane = iota((nq, lanes), 1)
        q_late = jnp.where((iota((nq, lanes), 0) // rows) % 2 == 1, last, 0)
        q_region = jnp.where(
            q_lane == 2 * heads, (1 - q_late).astype(F32),
            jnp.where(q_lane == 2 * heads + 1, q_late.astype(F32), 0.0),
        )
        low = q_lane < head_size
        sides = [
            jnp.where(low if e == 0 else ~low, 1.0, 0.0).astype(BF16) for e in (0, 1)
        ]
        ones_all = jnp.concatenate([ones] * (nk // pair_rows), 0)

        def one_pair(pair, carry):
            query = qs[pair, q0 : q0 + nq]
            keys = jnp.concatenate([ks[pair, k0 : k0 + nk], kx[k0 : k0 + nk]], 1)
            values = jnp.concatenate([vs[pair, k0 : k0 + nk], ones_all], 1)
            asked = [
                jnp.concatenate(
                    [
                        query * sides[e],
                        jnp.where(q_lane // 2 == 2 * pair + e, 1.0, q_region).astype(BF16),
                    ],
                    1,
                )
                for e in (0, 1)
            ]
            if nq == pair_rows:
                summed = dot(jnp.exp2(dot_t(jnp.concatenate(asked, 0), keys)).astype(BF16), values)
                parts = [summed[:nq], summed[nq:]]
            else:
                parts = [dot(jnp.exp2(dot_t(ask, keys)).astype(BF16), values) for ask in asked]
            ratios = []
            for e in (0, 1):
                if not first:
                    parts[e] = parts[e] + acc[pair, e]
                if not final:
                    acc[pair, e] = parts[e]
                else:
                    ratios.append(parts[e][:, :lanes] / parts[e][:, lanes:])
            if final:
                att[:nq, pl.ds(pl.multiple_of(pair * lanes, lanes), lanes)] = jnp.where(
                    low, ratios[0], ratios[1]
                ).astype(BF16)
            return carry

        with jax.named_scope("attend"):
            lax.fori_loop(0, pairs, one_pair, 0)

    lax.fori_loop(0, 2, project, 0)
    attend(0, half, 0, half, True, False)
    lax.fori_loop(2, 4, project, 0)
    weights[1].wait()

    for p in (3, 2):
        attend(p * pair_rows, pair_rows, 0, total, True, True)
        projected = dot(att[:pair_rows], wout[...]).astype(BF16)
        proj[p] = projected.reshape(2, rows, width)
        for rr in (1, 0):
            backward(1, p % 2, rr, start)
    attend(0, half, half, half, False, True)
    projected = dot(att[...], wout[...]).astype(BF16)
    proj[:2] = projected.reshape(2, 2, rows, width)
    for cc in (1, 0):
        for rr in (1, 0):
            backward(0, cc, rr, start)

    weights[2].wait()
    weights[3].wait()

    def join(step, carry):
        p = jnp.where(step < 2, step, 5 - step)
        with jax.named_scope("wait_back"):
            for rr in (0, 1):
                pltpu.make_async_copy(ret.at[p, rr], ret.at[p, rr], recv2.at[2 * p + rr]).wait()
        d, cc = p // 2, p % 2
        parity = parity_to(d, cc)
        r0, r1 = row_of(parity, 0), row_of(parity, 1)
        own = jnp.concatenate([x_ref[r0, 1 - cc], x_ref[r1, 1 - cc]], 0)
        back = ret[p].reshape(pair_rows, width)
        residual = (own.astype(F32) + back.astype(F32)).astype(BF16).astype(F32)
        mlp_in = layer_norm(residual).astype(BF16)
        joined = residual
        hidden_size = wup.shape[1]
        piece = 512
        for s in range(hidden_size // piece):
            up = dot(mlp_in, wup[:, s * piece : (s + 1) * piece])
            inner = math.sqrt(2.0 / math.pi) * (up + 0.044715 * (up * up * up))
            hidden = (0.5 * up * (1.0 + jnp.tanh(inner))).astype(BF16)
            joined = joined + dot(hidden, wdown[s * piece : (s + 1) * piece, :])
        joined = joined.astype(BF16)
        out_ref[r0, 1 - cc] = joined[:rows]
        out_ref[r1, 1 - cc] = joined[rows:]

        @pl.when(d == 1)
        def _():
            for k, r in enumerate((r0, r1)):
                ordered = dot(put, out_ref[r].reshape(2 * rows, width)).astype(BF16)
                for gl in range(groups * levels):
                    for i in range(SH_LAT):
                        lo = (gl * SH_LAT + i) * deep
                        outs[gl // levels, gl % levels, SH_LAT * r + i] = ordered[lo : lo + cells]
                deliver(r, 2 * cc + k).start()

        return carry

    def deliver(r, i):
        part = pl.ds(SH_LAT * r, SH_LAT)
        return pltpu.make_async_copy(outs.at[:, :, part], out_hbm.at[:, :, part], osem.at[i])

    token = iota((1, 2 * rows), 1)
    inside = token % rows
    place = jnp.where(
        inside < real, inside // SH_LON * deep + inside % SH_LON + token // rows * SH_LON, -1
    )
    put = jnp.where(iota((slabs * deep, 2 * rows), 0) == place, 1.0, 0.0).astype(BF16)

    lax.fori_loop(0, 4, join, 0)

    with jax.named_scope("drain"):
        for c in (0, 1):
            for r in range(4):
                forward(r, c, drain)
        for d in (0, 1):
            for cc in (0, 1):
                for rr in (0, 1):
                    backward(d, cc, rr, finish)
        for cc in (0, 1):
            for k in (0, 1):
                deliver(row_of(parity_to(1, cc), k), 2 * cc + k).wait()


def per_device(fields, surface_mask, w_qkv, w_out, logit_scale, mask_bias, w_up, w_down):
    groups, levels, nlat, nlon, width = fields.shape
    heads = logit_scale.shape[0]
    head_size = width // heads
    hidden_size = w_up.shape[1]
    tris, sides = nlat // SH_LAT, nlon // SH_LON
    real = groups * levels * SH_LAT * SH_LON
    rows = -(-(real + 1) // 16) * 16
    total = 8 * rows

    flags = surface_mask.reshape(levels, tris, SH_LAT, sides, SH_LON)
    flags = jnp.transpose(flags, (1, 3, 0, 2, 4)).reshape(tris, sides, 1, real // groups)
    flags = jnp.tile(flags.astype(BF16), (1, 1, 1, groups))
    flags = jnp.pad(
        flags, ((0, 0), (0, 0), (real - rows + 16, rows - real - 1), (0, 128 - real))
    )

    vmem = pl.BlockSpec(memory_space=pltpu.VMEM)
    scalars = pl.BlockSpec(memory_space=pltpu.SMEM)
    anywhere = pl.BlockSpec(memory_space=pl.ANY)
    return pl.pallas_call(
        functools.partial(kernel, real, heads),
        out_shape=jax.ShapeDtypeStruct(fields.shape, BF16),
        in_specs=[anywhere, vmem, scalars, scalars] + [anywhere] * 4,
        out_specs=anywhere,
        scratch_shapes=[
            pltpu.VMEM(fields.shape, BF16),
            pltpu.VMEM((tris, sides, rows, width), BF16),
            pltpu.VMEM(w_qkv.shape, BF16),
            pltpu.VMEM(w_out.shape, BF16),
            pltpu.VMEM(w_up.shape, BF16),
            pltpu.VMEM(w_down.shape, BF16),
            pltpu.VMEM((4, 2, rows, width), BF16),
            pltpu.VMEM((4, 2, rows, width), BF16),
            pltpu.VMEM((4, 2, rows, width), BF16),
            pltpu.VMEM((total // 2, width), BF16),
            pltpu.VMEM((heads // 2, total, 2 * head_size), BF16),
            pltpu.VMEM((heads // 2, total, 2 * head_size), BF16),
            pltpu.VMEM((heads // 2, total, 2 * head_size), BF16),
            pltpu.VMEM((total, 2 * head_size), BF16),
            pltpu.VMEM((heads // 2, 2, total // 2, 4 * head_size), F32),
            pltpu.VMEM((tris, sides, rows, width), BF16),
            pltpu.VMEM(fields.shape, BF16),
            pltpu.SemaphoreType.DMA((5,)),
            pltpu.SemaphoreType.DMA((4,)),
            pltpu.SemaphoreType.DMA((8,)),
            pltpu.SemaphoreType.DMA((8,)),
            pltpu.SemaphoreType.DMA((8,)),
            pltpu.SemaphoreType.DMA((8,)),
        ],
        compiler_params=pltpu.CompilerParams(
            collective_id=0, has_side_effects=True, vmem_limit_bytes=56 * 1024 * 1024
        ),
        name="window_block",
    )(fields, flags, logit_scale, mask_bias, w_qkv, w_out, w_up, w_down)


def solution(mesh):
    return jax.shard_map(
        per_device,
        mesh=mesh,
        in_specs=(
            P("grp", None, "lat", "lon", None),
            P(None, "lat", "lon"),
            P(),
            P(),
            P(),
            P(),
            P(),
            P(),
        ),
        out_specs=P("grp", None, "lat", "lon", None),
        check_vma=False,
    )
```

```python
import functools
import math

import jax
import jax.numpy as jnp
from jax import lax
from jax.experimental import pallas as pl
from jax.experimental.pallas import tpu as pltpu
from jax.sharding import PartitionSpec as P

SH_LAT = 3
SH_LON = 6
LOG2E = math.log2(math.e)
FAR = -30000.0
MESH = pl.DeviceIdType.MESH
BF16 = jnp.bfloat16
F32 = jnp.float32


def layer_norm(values):
    centred = values - jnp.mean(values, -1, keepdims=True)
    return centred * lax.rsqrt(jnp.mean(centred * centred, -1, keepdims=True) + 1e-05)


def iota(shape, axis):
    return lax.broadcasted_iota(jnp.int32, shape, axis)


def dot(left, right):
    return jnp.dot(left, right, preferred_element_type=F32)


def dot_t(left, right):
    return lax.dot_general(left, right, (((1,), (1,)), ((), ())), preferred_element_type=F32)


def kernel(
    real, heads,
    fields_hbm, mask_ref, scale_ref, bias_ref, wqkv_hbm, wout_hbm, wup_hbm, wdown_hbm,
    out_hbm,
    raw, tidy, x_ref, wqkv, wout, wup, wdown, win, ret, proj, att, qs, ks, vs, kx, acc, outs,
    wsem, osem, send1, recv1, send2, recv2,
):
    rows, width = x_ref.shape[2:]
    groups, nlat, lon_pairs, sub = raw.shape[:4]
    levels = mask_ref.shape[1]
    tiles = width // 128
    side_pairs = SH_LON // 2
    slab_rows = groups * SH_LAT * side_pairs * sub
    pair_rows = 2 * rows
    half = 2 * pair_rows
    total = 2 * half
    pairs = heads // 2
    head_size = width // heads
    lanes = 2 * head_size

    g, a, b = lax.axis_index("grp"), lax.axis_index("lat"), lax.axis_index("lon")
    na, nb = lax.axis_size("lat"), lax.axis_size("lon")

    barrier = pltpu.get_barrier_semaphore()
    greeted = 0
    for d in (0, 1):
        for da in (-1, 0, 1):
            for db in (-1, 0, 1):
                if d or da or db:
                    pl.semaphore_signal(
                        barrier,
                        inc=1,
                        device_id={
                            "grp": (g + d) % 2,
                            "lat": (a + da + na) % na,
                            "lon": (b + db + nb) % nb,
                        },
                        device_id_type=MESH,
                    )
                    greeted += 1
    load = pltpu.make_async_copy(fields_hbm, raw, wsem.at[4])
    load.start()
    weights = [
        pltpu.make_async_copy(src, dst, wsem.at[i])
        for i, (src, dst) in enumerate(
            ((wqkv_hbm, wqkv), (wout_hbm, wout), (wup_hbm, wup), (wdown_hbm, wdown))
        )
    ]
    for copy in weights:
        copy.start()

    def parity_to(d, cc):
        return (g + d + b + cc) % 2

    def row_of(parity, rr):
        return (1 + 2 * parity + rr) % 4

    def forward(r, c, act):
        parity, rr = (1, 1) if r == 0 else ((r - 1) // 2, (r - 1) % 2)
        cc = 1 - c
        d = (parity + g + b + cc) % 2
        p = 2 * d + cc
        src = x_ref.at[r, c]
        dst = win.at[p, rr]
        i = 2 * p + rr

        def local():
            return pltpu.make_async_copy(src, dst, recv1.at[i])

        def remote():
            return pltpu.make_async_remote_copy(
                src_ref=src, dst_ref=dst, send_sem=send1.at[i], recv_sem=recv1.at[i],
                device_id={
                    "grp": (g + d) % 2,
                    "lat": (a - 1 + na) % na if r == 0 else a,
                    "lon": (b - cc + nb) % nb,
                },
                device_id_type=MESH,
            )

        if r == 0 or cc:
            act(remote())
        else:
            pl.when(d == 1)(lambda: act(remote()))
            if act is begin:
                pl.when(d == 0)(lambda: act(local()))

    def begin(copy):
        copy.start()

    def drain(copy):
        copy.wait_send()

    def backward(d, cc, rr, act):
        parity = (g + b) % 2
        p = 2 * d + cc
        src = proj.at[p, rr]
        dst = ret.at[p, rr]
        i = 2 * p + rr
        edge = rr * parity

        def local():
            return pltpu.make_async_copy(src, dst, recv2.at[i])

        def remote():
            return pltpu.make_async_remote_copy(
                src_ref=src, dst_ref=dst, send_sem=send2.at[i], recv_sem=recv2.at[i],
                device_id={
                    "grp": (g + d) % 2,
                    "lat": (a + edge) % na,
                    "lon": (b + cc) % nb,
                },
                device_id_type=MESH,
            )

        act(d, cc, rr, parity, local, remote)

    def start(d, cc, rr, parity, local, remote):
        if d or cc:
            remote().start()
        elif rr == 0:
            local().start()
        else:
            pl.when(parity == 0)(lambda: local().start())
            pl.when(parity == 1)(lambda: remote().start())

    def finish(d, cc, rr, parity, local, remote):
        if d or cc:
            remote().wait_send()
        elif rr == 1:
            pl.when(parity == 1)(lambda: remote().wait_send())

    span_of = iota((tiles * rows, 1), 0)
    inside = span_of % rows
    place = jnp.where(
        inside < real,
        inside // levels * (tiles * levels) + span_of // rows * levels + inside % levels,
        -1,
    )
    pick = jnp.where(iota((tiles * rows, slab_rows), 1) == place, 1.0, 0.0).astype(BF16)

    tidy[...] = jnp.zeros_like(tidy)
    for i in range(nlat):
        tidy[levels * i : levels * (i + 1), : mask_ref.shape[2]] = mask_ref[i].astype(F32)
    spot = iota((8 * 128, 1), 0)
    block, inside = spot // 128, spot % 128
    cell = inside // levels
    at_lat = block // 2 * SH_LAT + cell // SH_LON % SH_LAT
    at_lat = at_lat * levels + inside % levels
    at_lon = block % 2 * SH_LON + cell % SH_LON
    at_lat = jnp.where(inside < real, at_lat, -1)
    by_lat = jnp.where(iota((8 * 128, tidy.shape[0]), 1) == at_lat, 1.0, 0.0).astype(BF16)
    by_cell = dot(by_lat, tidy[...].astype(BF16))
    by_cell = jnp.where(iota((8 * 128, 128), 1) == at_lon, by_cell, 0.0).astype(BF16)
    flags = dot_t(jnp.ones((16, 128), BF16), by_cell)
    flag_row = iota((16, 128), 0) == real - rows + 16

    with jax.named_scope("load"):
        load.wait()
    order = (0, 3, 1, 2)

    def sort_row(r):
        for c in (0, 1):
            piece = raw[:, SH_LAT * r : SH_LAT * (r + 1), side_pairs * c : side_pairs * (c + 1)]
            tall = dot(pick, piece.reshape(slab_rows, 128)).astype(BF16)
            for t in range(tiles):
                x_ref[r, c, :, 128 * t : 128 * (t + 1)] = tall[t * rows : (t + 1) * rows]
            k = 2 * r + c
            x_ref[r, c, rows - 16 :, :128] = jnp.where(
                flag_row,
                flags[:, 128 * k : 128 * (k + 1)],
                tall[rows - 16 : rows].astype(F32),
            ).astype(BF16)

    sort_row(order[0])
    with jax.named_scope("greet"):
        pl.semaphore_wait(barrier, greeted)
    for k in range(4):
        if k < 3:
            sort_row(order[k + 1])
        for c in (0, 1):
            forward(order[k], c, begin)

    last = jnp.where(a == na - 1, (g + b) % 2, 0)
    row_in_block = iota((pair_rows, lanes), 0) % rows
    valid = row_in_block < real
    lane = iota((pair_rows, lanes), 1)
    late = jnp.where(iota((pair_rows, lanes), 0) >= rows, last, 0)
    raw_bias = jnp.zeros((1, lanes), F32)
    qscale = jnp.zeros((1, width), F32)
    for h in range(heads):
        raw_bias = jnp.where(
            iota((1, lanes), 1) // 2 == h, bias_ref[h] * LOG2E, raw_bias
        )
        qscale = jnp.where(
            iota((1, width), 1) // head_size == h, scale_ref[h] * (LOG2E / head_size), qscale
        )
    bias_hi = raw_bias.astype(BF16).astype(F32)
    bias_row = jnp.where(iota(raw_bias.shape, 1) % 2 == 0, bias_hi, raw_bias - bias_hi)
    far = jnp.where(
        lane == 2 * heads, FAR * late.astype(F32),
        jnp.where(lane == 2 * heads + 1, FAR * (1 - late).astype(F32), 0.0),
    )
    span = 2 * lanes
    blocks = jnp.where(
        iota((span, span), 0) // head_size == iota((span, span), 1) // head_size,
        1.0 / head_size, 0.0,
    ).astype(BF16)
    eye = jnp.where(iota((rows, lanes), 0) == iota((rows, lanes), 1), 1.0, 0.0).astype(BF16)
    ones = jnp.where(valid, 1.0, 0.0).astype(BF16)

    with jax.named_scope("wait_w"):
        weights[0].wait()

    def project(p, carry):
        with jax.named_scope("wait_in"):
            for rr in (0, 1):
                pltpu.make_async_copy(win.at[p, rr], win.at[p, rr], recv1.at[2 * p + rr]).wait()
        both = win[p].reshape(pair_rows, width)
        normed = layer_norm(both.astype(F32)).astype(BF16)
        here = pl.ds(p * pair_rows, pair_rows)
        for part, store in ((0, qs), (1, ks)):
            for s in range(width // span):
                lo = s * span
                mixed = dot(normed, wqkv[:, part * width + lo : part * width + lo + span])
                square = dot((mixed * mixed).astype(BF16), blocks)
                unit = mixed * lax.rsqrt(square + 1e-06)
                if part == 0:
                    unit = unit * qscale[:, lo : lo + span]
                unit = unit.astype(BF16)
                store[2 * s, here] = unit[:, :lanes]
                store[2 * s + 1, here] = unit[:, lanes:]
        for s in range(width // span):
            lo = 2 * width + s * span
            mixed = dot(normed, wqkv[:, lo : lo + span])
            for k in (0, 1):
                vs[2 * s + k, here] = jnp.where(
                    valid, mixed[:, k * lanes : (k + 1) * lanes], 0.0
                ).astype(BF16)
        marks = jnp.concatenate(
            [
                dot_t(eye, jnp.broadcast_to(win[p, rr, real : real + 1, :lanes], (lanes, lanes)))
                for rr in (0, 1)
            ],
            0,
        )
        kx[here] = (marks * bias_row + far).astype(BF16)
        return carry

    def attend(q0, nq, k0, nk, first, final):
        q_lane = iota((nq, lanes), 1)
        q_late = jnp.where((iota((nq, lanes), 0) // rows) % 2 == 1, last, 0)
        q_region = jnp.where(
            q_lane == 2 * heads, (1 - q_late).astype(F32),
            jnp.where(q_lane == 2 * heads + 1, q_late.astype(F32), 0.0),
        )
        low = q_lane < head_size
        sides = [
            jnp.where(low if e == 0 else ~low, 1.0, 0.0).astype(BF16) for e in (0, 1)
        ]
        ones_all = jnp.concatenate([ones] * (nk // pair_rows), 0)

        def one_pair(pair, carry):
            query = qs[pair, q0 : q0 + nq]
            keys = jnp.concatenate([ks[pair, k0 : k0 + nk], kx[k0 : k0 + nk]], 1)
            values = jnp.concatenate([vs[pair, k0 : k0 + nk], ones_all], 1)
            asked = [
                jnp.concatenate(
                    [
                        query * sides[e],
                        jnp.where(q_lane // 2 == 2 * pair + e, 1.0, q_region).astype(BF16),
                    ],
                    1,
                )
                for e in (0, 1)
            ]
            if nq == pair_rows:
                summed = dot(jnp.exp2(dot_t(jnp.concatenate(asked, 0), keys)).astype(BF16), values)
                parts = [summed[:nq], summed[nq:]]
            else:
                parts = [dot(jnp.exp2(dot_t(ask, keys)).astype(BF16), values) for ask in asked]
            ratios = []
            for e in (0, 1):
                if not first:
                    parts[e] = parts[e] + acc[pair, e]
                if not final:
                    acc[pair, e] = parts[e]
                else:
                    ratios.append(parts[e][:, :lanes] / parts[e][:, lanes:])
            if final:
                att[:nq, pl.ds(pl.multiple_of(pair * lanes, lanes), lanes)] = jnp.where(
                    low, ratios[0], ratios[1]
                ).astype(BF16)
            return carry

        with jax.named_scope("attend"):
            lax.fori_loop(0, pairs, one_pair, 0)

    lax.fori_loop(0, 2, project, 0)
    attend(0, half, 0, half, True, False)
    lax.fori_loop(2, 4, project, 0)
    weights[1].wait()

    for p in (3, 2):
        attend(p * pair_rows, pair_rows, 0, total, True, True)
        projected = dot(att[:pair_rows], wout[...]).astype(BF16)
        proj[p] = projected.reshape(2, rows, width)
        for rr in (1, 0):
            backward(1, p % 2, rr, start)
    attend(0, half, half, half, False, True)
    projected = dot(att[...], wout[...]).astype(BF16)
    proj[:2] = projected.reshape(2, 2, rows, width)
    for cc in (1, 0):
        for rr in (1, 0):
            backward(0, cc, rr, start)

    weights[2].wait()
    weights[3].wait()

    def join(step, carry):
        p = jnp.where(step < 2, step, 5 - step)
        with jax.named_scope("wait_back"):
            for rr in (0, 1):
                pltpu.make_async_copy(ret.at[p, rr], ret.at[p, rr], recv2.at[2 * p + rr]).wait()
        d, cc = p // 2, p % 2
        parity = parity_to(d, cc)
        r0, r1 = row_of(parity, 0), row_of(parity, 1)
        own = jnp.concatenate([x_ref[r0, 1 - cc], x_ref[r1, 1 - cc]], 0)
        back = ret[p].reshape(pair_rows, width)
        residual = (own.astype(F32) + back.astype(F32)).astype(BF16).astype(F32)
        mlp_in = layer_norm(residual).astype(BF16)
        update = jnp.zeros_like(residual)
        hidden_size = wup.shape[1]
        piece = 512
        for s in range(hidden_size // piece):
            up = dot(mlp_in, wup[:, s * piece : (s + 1) * piece])
            slope = math.sqrt(2.0 / math.pi)
            bent = jnp.tanh(up * (slope + 0.044715 * slope * (up * up)))
            twice = (up + up * bent).astype(BF16)
            update = update + dot(twice, wdown[s * piece : (s + 1) * piece, :])
        joined = (residual + 0.5 * update).astype(BF16)
        for k, r in enumerate((r0, r1)):
            own_rows = joined[k * rows : (k + 1) * rows]
            tall = jnp.concatenate(
                [own_rows[:, 128 * t : 128 * (t + 1)] for t in range(tiles)], 0
            )
            i = 2 * p + k
            outs[i] = dot(put, tall).astype(BF16).reshape(outs.shape[1:])
            deliver(r, 1 - cc, i).start()
        return carry

    def deliver(r, c, i):
        rim = pl.ds(SH_LAT * r, SH_LAT)
        return pltpu.make_async_copy(
            outs.at[i], out_hbm.at[:, rim, pl.ds(side_pairs * c, side_pairs)], osem.at[i]
        )

    span_of = iota((1, tiles * rows), 1)
    inside = span_of % rows
    place = jnp.where(
        inside < real,
        inside // levels * (tiles * levels) + span_of // rows * levels + inside % levels,
        -1,
    )
    put = jnp.where(iota((slab_rows, tiles * rows), 0) == place, 1.0, 0.0).astype(BF16)

    lax.fori_loop(0, 4, join, 0)

    with jax.named_scope("drain"):
        for c in (0, 1):
            for r in range(4):
                forward(r, c, drain)
        for d in (0, 1):
            for cc in (0, 1):
                for rr in (0, 1):
                    backward(d, cc, rr, finish)
        for p in range(4):
            for k in (0, 1):
                r = row_of(parity_to(p // 2, p % 2), k)
                deliver(r, 1 - p % 2, 2 * p + k).wait()


def per_device(fields, surface_mask, w_qkv, w_out, logit_scale, mask_bias, w_up, w_down):
    groups, levels, nlat, nlon, width = fields.shape
    heads = logit_scale.shape[0]
    head_size = width // heads
    hidden_size = w_up.shape[1]
    tris, sides = nlat // SH_LAT, nlon // SH_LON
    real = groups * levels * SH_LAT * SH_LON
    rows = -(-(real + 1) // 16) * 16
    total = 8 * rows

    tiles = width // 128
    raw = fields.reshape(groups, levels, nlat, nlon, tiles, 128)
    raw = jnp.transpose(raw, (0, 2, 3, 4, 1, 5))
    raw = raw.reshape(groups, nlat, nlon // 2, 2 * tiles * levels, 128)

    vmem = pl.BlockSpec(memory_space=pltpu.VMEM)
    scalars = pl.BlockSpec(memory_space=pltpu.SMEM)
    anywhere = pl.BlockSpec(memory_space=pl.ANY)
    joined = pl.pallas_call(
        functools.partial(kernel, real, heads),
        out_shape=jax.ShapeDtypeStruct(raw.shape, BF16),
        in_specs=[anywhere, vmem, scalars, scalars] + [anywhere] * 4,
        out_specs=anywhere,
        scratch_shapes=[
            pltpu.VMEM(raw.shape, BF16),
            pltpu.VMEM((nlat * levels, 128), F32),
            pltpu.VMEM((tris, sides, rows, width), BF16),
            pltpu.VMEM(w_qkv.shape, BF16),
            pltpu.VMEM(w_out.shape, BF16),
            pltpu.VMEM(w_up.shape, BF16),
            pltpu.VMEM(w_down.shape, BF16),
            pltpu.VMEM((4, 2, rows, width), BF16),
            pltpu.VMEM((4, 2, rows, width), BF16),
            pltpu.VMEM((4, 2, rows, width), BF16),
            pltpu.VMEM((total // 2, width), BF16),
            pltpu.VMEM((heads // 2, total, 2 * head_size), BF16),
            pltpu.VMEM((heads // 2, total, 2 * head_size), BF16),
            pltpu.VMEM((heads // 2, total, 2 * head_size), BF16),
            pltpu.VMEM((total, 2 * head_size), BF16),
            pltpu.VMEM((heads // 2, 2, total // 2, 4 * head_size), F32),
            pltpu.VMEM((8, groups, SH_LAT, SH_LON // 2) + raw.shape[3:], BF16),
            pltpu.SemaphoreType.DMA((5,)),
            pltpu.SemaphoreType.DMA((8,)),
            pltpu.SemaphoreType.DMA((8,)),
            pltpu.SemaphoreType.DMA((8,)),
            pltpu.SemaphoreType.DMA((8,)),
            pltpu.SemaphoreType.DMA((8,)),
        ],
        compiler_params=pltpu.CompilerParams(
            collective_id=0, has_side_effects=True, vmem_limit_bytes=56 * 1024 * 1024
        ),
        name="window_block",
    )(raw, jnp.transpose(surface_mask, (1, 0, 2)), logit_scale, mask_bias, w_qkv, w_out, w_up, w_down)

    joined = joined.reshape(groups, nlat, nlon, tiles, levels, 128)
    return jnp.transpose(joined, (0, 4, 1, 2, 3, 5)).reshape(fields.shape)


def solution(mesh):
    return jax.shard_map(
        per_device,
        mesh=mesh,
        in_specs=(
            P("grp", None, "lat", "lon", None),
            P(None, "lat", "lon"),
            P(),
            P(),
            P(),
            P(),
            P(),
            P(),
        ),
        out_specs=P("grp", None, "lat", "lon", None),
        check_vma=False,
    )
```

```python
import functools
import math

import jax
import jax.numpy as jnp
from jax import lax
from jax.experimental import pallas as pl
from jax.experimental.pallas import tpu as pltpu
from jax.sharding import PartitionSpec as P

SH_LAT = 3
SH_LON = 6
LOG2E = math.log2(math.e)
FAR = -30000.0
MESH = pl.DeviceIdType.MESH
BF16 = jnp.bfloat16
F32 = jnp.float32


def layer_norm(values):
    centred = values - jnp.mean(values, -1, keepdims=True)
    return centred * lax.rsqrt(jnp.mean(centred * centred, -1, keepdims=True) + 1e-05)


def iota(shape, axis):
    return lax.broadcasted_iota(jnp.int32, shape, axis)


def dot(left, right):
    return jnp.dot(left, right, preferred_element_type=F32)


def dot_t(left, right):
    return lax.dot_general(left, right, (((1,), (1,)), ((), ())), preferred_element_type=F32)


def kernel(
    real, heads,
    fields_hbm, mask_ref, scale_ref, bias_ref, wqkv_hbm, wout_hbm, wup_hbm, wdown_hbm,
    out_hbm,
    raw, tidy, x_ref, wqkv, wout, wup, wdown, win, ret, proj, att, qs, ks, vs, kx, acc, outs,
    wsem, osem, send1, recv1, send2, recv2,
):
    rows, width = x_ref.shape[2:]
    groups, nlat, lon_pairs, sub = raw.shape[:4]
    levels = mask_ref.shape[1]
    tiles = width // 128
    side_pairs = SH_LON // 2
    slab_rows = groups * SH_LAT * side_pairs * sub
    pair_rows = 2 * rows
    half = 2 * pair_rows
    total = 2 * half
    pairs = heads // 2
    head_size = width // heads
    lanes = 2 * head_size

    g, a, b = lax.axis_index("grp"), lax.axis_index("lat"), lax.axis_index("lon")
    na, nb = lax.axis_size("lat"), lax.axis_size("lon")

    barrier = pltpu.get_barrier_semaphore()
    greeted = 0
    for d in (0, 1):
        for da in (-1, 0, 1):
            for db in (-1, 0, 1):
                if d or da or db:
                    pl.semaphore_signal(
                        barrier,
                        inc=1,
                        device_id={
                            "grp": (g + d) % 2,
                            "lat": (a + da + na) % na,
                            "lon": (b + db + nb) % nb,
                        },
                        device_id_type=MESH,
                    )
                    greeted += 1
    load = pltpu.make_async_copy(fields_hbm, raw, wsem.at[4])
    load.start()
    weights = [
        pltpu.make_async_copy(src, dst, wsem.at[i])
        for i, (src, dst) in enumerate(
            ((wqkv_hbm, wqkv), (wout_hbm, wout), (wup_hbm, wup), (wdown_hbm, wdown))
        )
    ]
    for copy in weights:
        copy.start()

    def parity_to(d, cc):
        return (g + d + b + cc) % 2

    def row_of(parity, rr):
        return (1 + 2 * parity + rr) % 4

    def forward(r, d, act):
        parity, rr = (1, 1) if r == 0 else ((r - 1) // 2, (r - 1) % 2)
        cc = (parity + g + b + d) % 2
        p = 2 * d + cc
        src = x_ref.at[r, 1 - cc]
        dst = win.at[p, rr]
        i = 2 * p + rr

        def local():
            return pltpu.make_async_copy(src, dst, recv1.at[i])

        def remote():
            return pltpu.make_async_remote_copy(
                src_ref=src, dst_ref=dst, send_sem=send1.at[i], recv_sem=recv1.at[i],
                device_id={
                    "grp": (g + d) % 2,
                    "lat": (a - 1 + na) % na if r == 0 else a,
                    "lon": (b - cc + nb) % nb,
                },
                device_id_type=MESH,
            )

        if r == 0 or d:
            act(remote())
        else:
            pl.when(cc == 1)(lambda: act(remote()))
            if act is begin:
                pl.when(cc == 0)(lambda: act(local()))

    def begin(copy):
        copy.start()

    def drain(copy):
        copy.wait_send()

    def backward(d, cc, rr, act):
        parity = (g + b) % 2
        p = 2 * d + cc
        src = proj.at[p, rr]
        dst = ret.at[p, rr]
        i = 2 * p + rr
        edge = rr * parity

        def local():
            return pltpu.make_async_copy(src, dst, recv2.at[i])

        def remote():
            return pltpu.make_async_remote_copy(
                src_ref=src, dst_ref=dst, send_sem=send2.at[i], recv_sem=recv2.at[i],
                device_id={
                    "grp": (g + d) % 2,
                    "lat": (a + edge) % na,
                    "lon": (b + cc) % nb,
                },
                device_id_type=MESH,
            )

        act(d, cc, rr, parity, local, remote)

    def start(d, cc, rr, parity, local, remote):
        if d or cc:
            remote().start()
        elif rr == 0:
            local().start()
        else:
            pl.when(parity == 0)(lambda: local().start())
            pl.when(parity == 1)(lambda: remote().start())

    def finish(d, cc, rr, parity, local, remote):
        if d or cc:
            remote().wait_send()
        elif rr == 1:
            pl.when(parity == 1)(lambda: remote().wait_send())

    span_of = iota((tiles * rows, 1), 0)
    inside = span_of % rows
    place = jnp.where(
        inside < real,
        inside // levels * (tiles * levels) + span_of // rows * levels + inside % levels,
        -1,
    )
    pick = jnp.where(iota((tiles * rows, slab_rows), 1) == place, 1.0, 0.0).astype(BF16)

    tidy[...] = jnp.zeros_like(tidy)
    for i in range(nlat):
        tidy[levels * i : levels * (i + 1), : mask_ref.shape[2]] = mask_ref[i].astype(F32)
    spot = iota((8 * 128, 1), 0)
    block, inside = spot // 128, spot % 128
    cell = inside // levels
    at_lat = block // 2 * SH_LAT + cell // SH_LON % SH_LAT
    at_lat = at_lat * levels + inside % levels
    at_lon = block % 2 * SH_LON + cell % SH_LON
    at_lat = jnp.where(inside < real, at_lat, -1)
    by_lat = jnp.where(iota((8 * 128, tidy.shape[0]), 1) == at_lat, 1.0, 0.0).astype(BF16)
    by_cell = dot(by_lat, tidy[...].astype(BF16))
    by_cell = jnp.where(iota((8 * 128, 128), 1) == at_lon, by_cell, 0.0).astype(BF16)
    flags = dot_t(jnp.ones((16, 128), BF16), by_cell)
    flag_row = iota((16, 128), 0) == real - rows + 16

    with jax.named_scope("load"):
        load.wait()
    order = (0, 3, 1, 2)

    def sort_row(r):
        for c in (0, 1):
            piece = raw[:, SH_LAT * r : SH_LAT * (r + 1), side_pairs * c : side_pairs * (c + 1)]
            tall = dot(pick, piece.reshape(slab_rows, 128)).astype(BF16)
            for t in range(tiles):
                x_ref[r, c, :, 128 * t : 128 * (t + 1)] = tall[t * rows : (t + 1) * rows]
            k = 2 * r + c
            x_ref[r, c, rows - 16 :, :128] = jnp.where(
                flag_row,
                flags[:, 128 * k : 128 * (k + 1)],
                tall[rows - 16 : rows].astype(F32),
            ).astype(BF16)

    sort_row(order[0])
    with jax.named_scope("greet"):
        pl.semaphore_wait(barrier, greeted)
    for k in range(4):
        if k < 3:
            sort_row(order[k + 1])
        forward(order[k], 0, begin)
        if k:
            forward(order[k - 1], 1, begin)
    forward(order[3], 1, begin)

    last = jnp.where(a == na - 1, (g + b) % 2, 0)
    row_in_block = iota((pair_rows, lanes), 0) % rows
    valid = row_in_block < real
    lane = iota((pair_rows, lanes), 1)
    late = jnp.where(iota((pair_rows, lanes), 0) >= rows, last, 0)
    raw_bias = jnp.zeros((1, lanes), F32)
    qscale = jnp.zeros((1, width), F32)
    for h in range(heads):
        raw_bias = jnp.where(
            iota((1, lanes), 1) // 2 == h, bias_ref[h] * LOG2E, raw_bias
        )
        qscale = jnp.where(
            iota((1, width), 1) // head_size == h, scale_ref[h] * (LOG2E / head_size), qscale
        )
    bias_hi = raw_bias.astype(BF16).astype(F32)
    bias_row = jnp.where(iota(raw_bias.shape, 1) % 2 == 0, bias_hi, raw_bias - bias_hi)
    far = jnp.where(
        lane == 2 * heads, FAR * late.astype(F32),
        jnp.where(lane == 2 * heads + 1, FAR * (1 - late).astype(F32), 0.0),
    )
    span = 2 * lanes
    blocks = jnp.where(
        iota((span, span), 0) // head_size == iota((span, span), 1) // head_size,
        1.0 / head_size, 0.0,
    ).astype(BF16)
    eye = jnp.where(iota((rows, lanes), 0) == iota((rows, lanes), 1), 1.0, 0.0).astype(BF16)
    ones = jnp.where(valid, 1.0, 0.0).astype(BF16)

    with jax.named_scope("wait_w"):
        weights[0].wait()

    def project(p, carry):
        with jax.named_scope("wait_in"):
            for rr in (0, 1):
                pltpu.make_async_copy(win.at[p, rr], win.at[p, rr], recv1.at[2 * p + rr]).wait()
        both = win[p].reshape(pair_rows, width)
        normed = layer_norm(both.astype(F32)).astype(BF16)
        here = pl.ds(p * pair_rows, pair_rows)
        for part, store in ((0, qs), (1, ks)):
            for s in range(width // span):
                lo = s * span
                mixed = dot(normed, wqkv[:, part * width + lo : part * width + lo + span])
                square = dot((mixed * mixed).astype(BF16), blocks)
                unit = mixed * lax.rsqrt(square + 1e-06)
                if part == 0:
                    unit = unit * qscale[:, lo : lo + span]
                unit = unit.astype(BF16)
                store[2 * s, here] = unit[:, :lanes]
                store[2 * s + 1, here] = unit[:, lanes:]
        for s in range(width // span):
            lo = 2 * width + s * span
            mixed = dot(normed, wqkv[:, lo : lo + span])
            for k in (0, 1):
                vs[2 * s + k, here] = jnp.where(
                    valid, mixed[:, k * lanes : (k + 1) * lanes], 0.0
                ).astype(BF16)
        marks = jnp.concatenate(
            [
                dot_t(eye, jnp.broadcast_to(win[p, rr, real : real + 1, :lanes], (lanes, lanes)))
                for rr in (0, 1)
            ],
            0,
        )
        kx[here] = (marks * bias_row + far).astype(BF16)
        return carry

    def attend(q0, nq, k0, nk, first, final):
        q_lane = iota((nq, lanes), 1)
        q_late = jnp.where((iota((nq, lanes), 0) // rows) % 2 == 1, last, 0)
        q_region = jnp.where(
            q_lane == 2 * heads, (1 - q_late).astype(F32),
            jnp.where(q_lane == 2 * heads + 1, q_late.astype(F32), 0.0),
        )
        low = q_lane < head_size
        sides = [
            jnp.where(low if e == 0 else ~low, 1.0, 0.0).astype(BF16) for e in (0, 1)
        ]
        ones_all = jnp.concatenate([ones] * (nk // pair_rows), 0)

        def one_pair(pair, carry):
            query = qs[pair, q0 : q0 + nq]
            keys = jnp.concatenate([ks[pair, k0 : k0 + nk], kx[k0 : k0 + nk]], 1)
            values = jnp.concatenate([vs[pair, k0 : k0 + nk], ones_all], 1)
            asked = [
                jnp.concatenate(
                    [
                        query * sides[e],
                        jnp.where(q_lane // 2 == 2 * pair + e, 1.0, q_region).astype(BF16),
                    ],
                    1,
                )
                for e in (0, 1)
            ]
            if nq == pair_rows:
                summed = dot(jnp.exp2(dot_t(jnp.concatenate(asked, 0), keys)).astype(BF16), values)
                parts = [summed[:nq], summed[nq:]]
            else:
                parts = [dot(jnp.exp2(dot_t(ask, keys)).astype(BF16), values) for ask in asked]
            ratios = []
            for e in (0, 1):
                if not first:
                    parts[e] = parts[e] + acc[pair, e]
                if not final:
                    acc[pair, e] = parts[e]
                else:
                    ratios.append(parts[e][:, :lanes] / parts[e][:, lanes:])
            if final:
                att[:nq, pl.ds(pl.multiple_of(pair * lanes, lanes), lanes)] = jnp.where(
                    low, ratios[0], ratios[1]
                ).astype(BF16)
            return carry

        with jax.named_scope("attend"):
            lax.fori_loop(0, pairs, one_pair, 0)

    lax.fori_loop(0, 2, project, 0)
    attend(0, half, 0, half, True, False)
    lax.fori_loop(2, 4, project, 0)
    weights[1].wait()

    def far_queries(p):
        attend(p * pair_rows, pair_rows, 0, total, True, True)
        projected = dot(att[:pair_rows], wout[...]).astype(BF16)
        proj[p] = projected.reshape(2, rows, width)
        for rr in (1, 0):
            backward(1, p % 2, rr, start)

    far_queries(3)
    attend(0, half, half, half, False, True)
    projected = dot(att[...], wout[...]).astype(BF16)
    proj[:2] = projected.reshape(2, 2, rows, width)
    for cc in (1, 0):
        for rr in (1, 0):
            backward(0, cc, rr, start)
    far_queries(2)

    weights[2].wait()
    weights[3].wait()

    def join(step, carry):
        p = jnp.where(step < 2, step, 5 - step)
        with jax.named_scope("wait_back"):
            for rr in (0, 1):
                pltpu.make_async_copy(ret.at[p, rr], ret.at[p, rr], recv2.at[2 * p + rr]).wait()
        d, cc = p // 2, p % 2
        parity = parity_to(d, cc)
        r0, r1 = row_of(parity, 0), row_of(parity, 1)
        own = jnp.concatenate([x_ref[r0, 1 - cc], x_ref[r1, 1 - cc]], 0)
        back = ret[p].reshape(pair_rows, width)
        residual = (own.astype(F32) + back.astype(F32)).astype(BF16).astype(F32)
        mlp_in = layer_norm(residual).astype(BF16)
        update = jnp.zeros_like(residual)
        hidden_size = wup.shape[1]
        piece = 512
        for s in range(hidden_size // piece):
            up = dot(mlp_in, wup[:, s * piece : (s + 1) * piece])
            slope = math.sqrt(2.0 / math.pi)
            bent = jnp.tanh(up * (slope + 0.044715 * slope * (up * up)))
            twice = (up + up * bent).astype(BF16)
            update = update + dot(twice, wdown[s * piece : (s + 1) * piece, :])
        joined = (residual + 0.5 * update).astype(BF16)
        for k, r in enumerate((r0, r1)):
            own_rows = joined[k * rows : (k + 1) * rows]
            tall = jnp.concatenate(
                [own_rows[:, 128 * t : 128 * (t + 1)] for t in range(tiles)], 0
            )
            i = 2 * p + k
            outs[i] = dot(put, tall).astype(BF16).reshape(outs.shape[1:])
            deliver(r, 1 - cc, i).start()
        return carry

    def deliver(r, c, i):
        rim = pl.ds(SH_LAT * r, SH_LAT)
        return pltpu.make_async_copy(
            outs.at[i], out_hbm.at[:, rim, pl.ds(side_pairs * c, side_pairs)], osem.at[i]
        )

    span_of = iota((1, tiles * rows), 1)
    inside = span_of % rows
    place = jnp.where(
        inside < real,
        inside // levels * (tiles * levels) + span_of // rows * levels + inside % levels,
        -1,
    )
    put = jnp.where(iota((slab_rows, tiles * rows), 0) == place, 1.0, 0.0).astype(BF16)

    lax.fori_loop(0, 4, join, 0)

    with jax.named_scope("drain"):
        for d in (0, 1):
            for r in range(4):
                forward(r, d, drain)
        for d in (0, 1):
            for cc in (0, 1):
                for rr in (0, 1):
                    backward(d, cc, rr, finish)
        for p in range(4):
            for k in (0, 1):
                r = row_of(parity_to(p // 2, p % 2), k)
                deliver(r, 1 - p % 2, 2 * p + k).wait()


def hand_over(src, dst, held, in_sem, out_sem):
    takes = [pltpu.make_async_copy(src.at[i], held.at[i], in_sem.at[i]) for i in range(src.shape[0])]
    gives = [pltpu.make_async_copy(held.at[i], dst.at[i], out_sem.at[i]) for i in range(src.shape[0])]
    for take in takes:
        take.start()
    for take, give in zip(takes, gives):
        take.wait()
        give.start()
    for give in gives:
        give.wait()


def per_device(fields, surface_mask, w_qkv, w_out, logit_scale, mask_bias, w_up, w_down):
    groups, levels, nlat, nlon, width = fields.shape
    heads = logit_scale.shape[0]
    head_size = width // heads
    hidden_size = w_up.shape[1]
    tris, sides = nlat // SH_LAT, nlon // SH_LON
    real = groups * levels * SH_LAT * SH_LON
    rows = -(-(real + 1) // 16) * 16
    total = 8 * rows

    tiles = width // 128
    raw = fields.reshape(groups, levels, nlat, nlon, tiles, 128)
    raw = jnp.transpose(raw, (0, 2, 3, 4, 1, 5))
    raw = raw.reshape(groups, nlat, nlon // 2, 2 * tiles * levels, 128)

    vmem = pl.BlockSpec(memory_space=pltpu.VMEM)
    scalars = pl.BlockSpec(memory_space=pltpu.SMEM)
    anywhere = pl.BlockSpec(memory_space=pl.ANY)
    joined = pl.pallas_call(
        functools.partial(kernel, real, heads),
        out_shape=jax.ShapeDtypeStruct(raw.shape, BF16),
        in_specs=[anywhere, vmem, scalars, scalars] + [anywhere] * 4,
        out_specs=anywhere,
        scratch_shapes=[
            pltpu.VMEM(raw.shape, BF16),
            pltpu.VMEM((nlat * levels, 128), F32),
            pltpu.VMEM((tris, sides, rows, width), BF16),
            pltpu.VMEM(w_qkv.shape, BF16),
            pltpu.VMEM(w_out.shape, BF16),
            pltpu.VMEM(w_up.shape, BF16),
            pltpu.VMEM(w_down.shape, BF16),
            pltpu.VMEM((4, 2, rows, width), BF16),
            pltpu.VMEM((4, 2, rows, width), BF16),
            pltpu.VMEM((4, 2, rows, width), BF16),
            pltpu.VMEM((total // 2, width), BF16),
            pltpu.VMEM((heads // 2, total, 2 * head_size), BF16),
            pltpu.VMEM((heads // 2, total, 2 * head_size), BF16),
            pltpu.VMEM((heads // 2, total, 2 * head_size), BF16),
            pltpu.VMEM((total, 2 * head_size), BF16),
            pltpu.VMEM((heads // 2, 2, total // 2, 4 * head_size), F32),
            pltpu.VMEM((8, groups, SH_LAT, SH_LON // 2) + raw.shape[3:], BF16),
            pltpu.SemaphoreType.DMA((5,)),
            pltpu.SemaphoreType.DMA((8,)),
            pltpu.SemaphoreType.DMA((8,)),
            pltpu.SemaphoreType.DMA((8,)),
            pltpu.SemaphoreType.DMA((8,)),
            pltpu.SemaphoreType.DMA((8,)),
        ],
        compiler_params=pltpu.CompilerParams(
            collective_id=0, has_side_effects=True, vmem_limit_bytes=56 * 1024 * 1024
        ),
        name="window_block",
    )(raw, jnp.transpose(surface_mask, (1, 0, 2)), logit_scale, mask_bias, w_qkv, w_out, w_up, w_down)

    joined = pl.pallas_call(
        hand_over,
        out_shape=jax.ShapeDtypeStruct(raw.shape, BF16),
        in_specs=[anywhere],
        out_specs=anywhere,
        scratch_shapes=[
            pltpu.VMEM(raw.shape, BF16),
            pltpu.SemaphoreType.DMA((groups,)),
            pltpu.SemaphoreType.DMA((groups,)),
        ],
        name="hand_over",
    )(joined)
    joined = joined.reshape(groups, nlat, nlon, tiles, levels, 128)
    return jnp.transpose(joined, (0, 4, 1, 2, 3, 5)).reshape(fields.shape)


def solution(mesh):
    return jax.shard_map(
        per_device,
        mesh=mesh,
        in_specs=(
            P("grp", None, "lat", "lon", None),
            P(None, "lat", "lon"),
            P(),
            P(),
            P(),
            P(),
            P(),
            P(),
        ),
        out_specs=P("grp", None, "lat", "lon", None),
        check_vma=False,
    )
```

```python
import functools
import math

import jax
import jax.numpy as jnp
from jax import lax
from jax.experimental import pallas as pl
from jax.experimental.pallas import tpu as pltpu
from jax.sharding import PartitionSpec as P

SH_LAT = 3
SH_LON = 6
LOG2E = math.log2(math.e)
FAR = -30000.0
MESH = pl.DeviceIdType.MESH
BF16 = jnp.bfloat16
F32 = jnp.float32


def layer_norm(values):
    centred = values - jnp.mean(values, -1, keepdims=True)
    return centred * lax.rsqrt(jnp.mean(centred * centred, -1, keepdims=True) + 1e-05)


def iota(shape, axis):
    return lax.broadcasted_iota(jnp.int32, shape, axis)


def dot(left, right):
    return jnp.dot(left, right, preferred_element_type=F32)


def dot_t(left, right):
    return lax.dot_general(left, right, (((1,), (1,)), ((), ())), preferred_element_type=F32)


def kernel(
    real, heads,
    fields_hbm, mask_ref, scale_ref, bias_ref, wqkv_hbm, wout_hbm, wup_hbm, wdown_hbm,
    out_hbm,
    raw, tidy, x_ref, wqkv, wout, wup, wdown, win, ret, proj, att, qs, ks, vs, kx, acc, outs,
    wsem, osem, send1, recv1, send2, recv2,
):
    rows, width = x_ref.shape[2:]
    groups, nlat, lon_pairs, sub = raw.shape[:4]
    levels = mask_ref.shape[1]
    tiles = width // 128
    side_pairs = SH_LON // 2
    slab_rows = groups * SH_LAT * side_pairs * sub
    pair_rows = 2 * rows
    half = 2 * pair_rows
    total = 2 * half
    pairs = heads // 2
    head_size = width // heads
    lanes = 2 * head_size

    g, a, b = lax.axis_index("grp"), lax.axis_index("lat"), lax.axis_index("lon")
    na, nb = lax.axis_size("lat"), lax.axis_size("lon")

    barrier = pltpu.get_barrier_semaphore()
    greeted = 0
    for d in (0, 1):
        for da in (-1, 0, 1):
            for db in (-1, 0, 1):
                if d or da or db:
                    pl.semaphore_signal(
                        barrier,
                        inc=1,
                        device_id={
                            "grp": (g + d) % 2,
                            "lat": (a + da + na) % na,
                            "lon": (b + db + nb) % nb,
                        },
                        device_id_type=MESH,
                    )
                    greeted += 1
    load = pltpu.make_async_copy(fields_hbm, raw, wsem.at[4])
    load.start()
    weights = [
        pltpu.make_async_copy(src, dst, wsem.at[i])
        for i, (src, dst) in enumerate(
            ((wqkv_hbm, wqkv), (wout_hbm, wout), (wup_hbm, wup), (wdown_hbm, wdown))
        )
    ]
    for copy in weights:
        copy.start()

    def parity_to(d, cc):
        return (g + d + b + cc) % 2

    def row_of(parity, rr):
        return (1 + 2 * parity + rr) % 4

    def forward(r, d, act):
        parity, rr = (1, 1) if r == 0 else ((r - 1) // 2, (r - 1) % 2)
        cc = (parity + g + b + d) % 2
        p = 2 * d + cc
        src = x_ref.at[r, 1 - cc]
        dst = win.at[p, rr]
        i = 2 * p + rr

        def local():
            return pltpu.make_async_copy(src, dst, recv1.at[i])

        def remote():
            return pltpu.make_async_remote_copy(
                src_ref=src, dst_ref=dst, send_sem=send1.at[i], recv_sem=recv1.at[i],
                device_id={
                    "grp": (g + d) % 2,
                    "lat": (a - 1 + na) % na if r == 0 else a,
                    "lon": (b - cc + nb) % nb,
                },
                device_id_type=MESH,
            )

        if r == 0 or d:
            act(remote())
        else:
            pl.when(cc == 1)(lambda: act(remote()))
            if act is begin:
                pl.when(cc == 0)(lambda: act(local()))

    def begin(copy):
        copy.start()

    def drain(copy):
        copy.wait_send()

    def backward(d, cc, rr, act):
        parity = (g + b) % 2
        p = 2 * d + cc
        src = proj.at[p, rr]
        dst = ret.at[p, rr]
        i = 2 * p + rr
        edge = rr * parity

        def local():
            return pltpu.make_async_copy(src, dst, recv2.at[i])

        def remote():
            return pltpu.make_async_remote_copy(
                src_ref=src, dst_ref=dst, send_sem=send2.at[i], recv_sem=recv2.at[i],
                device_id={
                    "grp": (g + d) % 2,
                    "lat": (a + edge) % na,
                    "lon": (b + cc) % nb,
                },
                device_id_type=MESH,
            )

        act(d, cc, rr, parity, local, remote)

    def start(d, cc, rr, parity, local, remote):
        if d or cc:
            remote().start()
        elif rr == 0:
            local().start()
        else:
            pl.when(parity == 0)(lambda: local().start())
            pl.when(parity == 1)(lambda: remote().start())

    def finish(d, cc, rr, parity, local, remote):
        if d or cc:
            remote().wait_send()
        elif rr == 1:
            pl.when(parity == 1)(lambda: remote().wait_send())

    span_of = iota((tiles * rows, 1), 0)
    inside = span_of % rows
    place = jnp.where(
        inside < real,
        inside // levels * (tiles * levels) + span_of // rows * levels + inside % levels,
        -1,
    )
    pick = jnp.where(iota((tiles * rows, slab_rows), 1) == place, 1.0, 0.0).astype(BF16)

    tidy[...] = jnp.zeros_like(tidy)
    for i in range(nlat):
        tidy[levels * i : levels * (i + 1), : mask_ref.shape[2]] = mask_ref[i].astype(F32)
    spot = iota((8 * 128, 1), 0)
    block, inside = spot // 128, spot % 128
    cell = inside // levels
    at_lat = block // 2 * SH_LAT + cell // SH_LON % SH_LAT
    at_lat = at_lat * levels + inside % levels
    at_lon = block % 2 * SH_LON + cell % SH_LON
    at_lat = jnp.where(inside < real, at_lat, -1)
    by_lat = jnp.where(iota((8 * 128, tidy.shape[0]), 1) == at_lat, 1.0, 0.0).astype(BF16)
    by_cell = dot(by_lat, tidy[...].astype(BF16))
    by_cell = jnp.where(iota((8 * 128, 128), 1) == at_lon, by_cell, 0.0).astype(BF16)
    flags = dot_t(jnp.ones((16, 128), BF16), by_cell)
    flag_row = iota((16, 128), 0) == real - rows + 16

    with jax.named_scope("load"):
        load.wait()

    def sort_row(r):
        for c in (0, 1):
            piece = raw[:, SH_LAT * r : SH_LAT * (r + 1), side_pairs * c : side_pairs * (c + 1)]
            tall = dot(pick, piece.reshape(slab_rows, 128)).astype(BF16)
            for t in range(tiles):
                x_ref[r, c, :, 128 * t : 128 * (t + 1)] = tall[t * rows : (t + 1) * rows]
            k = 2 * r + c
            x_ref[r, c, rows - 16 :, :128] = jnp.where(
                flag_row,
                flags[:, 128 * k : 128 * (k + 1)],
                tall[rows - 16 : rows].astype(F32),
            ).astype(BF16)

    sort_row(0)
    with jax.named_scope("greet"):
        pl.semaphore_wait(barrier, greeted)
    for r in range(4):
        if r < 3:
            sort_row(r + 1)
        forward(r, 0, begin)
        if r > 1:
            forward(r - 1, 1, begin)
    forward(0, 1, begin)
    forward(3, 1, begin)

    last = jnp.where(a == na - 1, (g + b) % 2, 0)
    row_in_block = iota((pair_rows, lanes), 0) % rows
    valid = row_in_block < real
    lane = iota((pair_rows, lanes), 1)
    late = jnp.where(iota((pair_rows, lanes), 0) >= rows, last, 0)
    raw_bias = jnp.zeros((1, lanes), F32)
    qscale = jnp.zeros((1, width), F32)
    for h in range(heads):
        raw_bias = jnp.where(
            iota((1, lanes), 1) // 2 == h, bias_ref[h] * LOG2E, raw_bias
        )
        qscale = jnp.where(
            iota((1, width), 1) // head_size == h, scale_ref[h] * (LOG2E / head_size), qscale
        )
    bias_hi = raw_bias.astype(BF16).astype(F32)
    bias_row = jnp.where(iota(raw_bias.shape, 1) % 2 == 0, bias_hi, raw_bias - bias_hi)
    far = jnp.where(
        lane == 2 * heads, FAR * late.astype(F32),
        jnp.where(lane == 2 * heads + 1, FAR * (1 - late).astype(F32), 0.0),
    )
    span = 2 * lanes
    blocks = jnp.where(
        iota((span, span), 0) // head_size == iota((span, span), 1) // head_size,
        1.0 / head_size, 0.0,
    ).astype(BF16)
    eye = jnp.where(iota((rows, lanes), 0) == iota((rows, lanes), 1), 1.0, 0.0).astype(BF16)
    ones = jnp.where(valid, 1.0, 0.0).astype(BF16)

    with jax.named_scope("wait_w"):
        weights[0].wait()

    def project(p, carry):
        with jax.named_scope("wait_in"):
            for rr in (0, 1):
                pltpu.make_async_copy(win.at[p, rr], win.at[p, rr], recv1.at[2 * p + rr]).wait()
        both = win[p].reshape(pair_rows, width)
        normed = layer_norm(both.astype(F32)).astype(BF16)
        here = pl.ds(p * pair_rows, pair_rows)
        for part, store in ((0, qs), (1, ks)):
            for s in range(width // span):
                lo = s * span
                mixed = dot(normed, wqkv[:, part * width + lo : part * width + lo + span])
                square = dot((mixed * mixed).astype(BF16), blocks)
                unit = mixed * lax.rsqrt(square + 1e-06)
                if part == 0:
                    unit = unit * qscale[:, lo : lo + span]
                unit = unit.astype(BF16)
                store[2 * s, here] = unit[:, :lanes]
                store[2 * s + 1, here] = unit[:, lanes:]
        for s in range(width // span):
            lo = 2 * width + s * span
            mixed = dot(normed, wqkv[:, lo : lo + span])
            for k in (0, 1):
                vs[2 * s + k, here] = jnp.where(
                    valid, mixed[:, k * lanes : (k + 1) * lanes], 0.0
                ).astype(BF16)
        marks = jnp.concatenate(
            [
                dot_t(eye, jnp.broadcast_to(win[p, rr, real : real + 1, :lanes], (lanes, lanes)))
                for rr in (0, 1)
            ],
            0,
        )
        kx[here] = (marks * bias_row + far).astype(BF16)
        return carry

    def attend(q0, nq, k0, nk, first, final):
        q_lane = iota((nq, lanes), 1)
        q_late = jnp.where((iota((nq, lanes), 0) // rows) % 2 == 1, last, 0)
        q_region = jnp.where(
            q_lane == 2 * heads, (1 - q_late).astype(F32),
            jnp.where(q_lane == 2 * heads + 1, q_late.astype(F32), 0.0),
        )
        low = q_lane < head_size
        sides = [
            jnp.where(low if e == 0 else ~low, 1.0, 0.0).astype(BF16) for e in (0, 1)
        ]
        ones_all = jnp.concatenate([ones] * (nk // pair_rows), 0)

        def one_pair(pair, carry):
            query = qs[pair, q0 : q0 + nq]
            keys = jnp.concatenate([ks[pair, k0 : k0 + nk], kx[k0 : k0 + nk]], 1)
            values = jnp.concatenate([vs[pair, k0 : k0 + nk], ones_all], 1)
            asked = [
                jnp.concatenate(
                    [
                        query * sides[e],
                        jnp.where(q_lane // 2 == 2 * pair + e, 1.0, q_region).astype(BF16),
                    ],
                    1,
                )
                for e in (0, 1)
            ]
            if nq == pair_rows:
                summed = dot(jnp.exp2(dot_t(jnp.concatenate(asked, 0), keys)).astype(BF16), values)
                parts = [summed[:nq], summed[nq:]]
            else:
                parts = [dot(jnp.exp2(dot_t(ask, keys)).astype(BF16), values) for ask in asked]
            ratios = []
            for e in (0, 1):
                if not first:
                    parts[e] = parts[e] + acc[pair, e]
                if not final:
                    acc[pair, e] = parts[e]
                else:
                    ratios.append(parts[e][:, :lanes] / parts[e][:, lanes:])
            if final:
                att[:nq, pl.ds(pl.multiple_of(pair * lanes, lanes), lanes)] = jnp.where(
                    low, ratios[0], ratios[1]
                ).astype(BF16)
            return carry

        with jax.named_scope("attend"):
            lax.fori_loop(0, pairs, one_pair, 0)

    lax.fori_loop(0, 2, project, 0)
    attend(0, half, 0, half, True, False)
    lax.fori_loop(2, 4, project, 0)
    weights[1].wait()

    def far_queries(p):
        attend(p * pair_rows, pair_rows, 0, total, True, True)
        projected = dot(att[:pair_rows], wout[...]).astype(BF16)
        proj[p] = projected.reshape(2, rows, width)
        for rr in (1, 0):
            backward(1, p % 2, rr, start)

    far_queries(3)
    attend(0, half, half, half, False, True)
    projected = dot(att[...], wout[...]).astype(BF16)
    proj[:2] = projected.reshape(2, 2, rows, width)
    for cc in (1, 0):
        for rr in (1, 0):
            backward(0, cc, rr, start)
    far_queries(2)

    weights[2].wait()
    weights[3].wait()

    def join(step, carry):
        p = jnp.where(step < 2, step, 5 - step)
        with jax.named_scope("wait_back"):
            for rr in (0, 1):
                pltpu.make_async_copy(ret.at[p, rr], ret.at[p, rr], recv2.at[2 * p + rr]).wait()
        d, cc = p // 2, p % 2
        parity = parity_to(d, cc)
        r0, r1 = row_of(parity, 0), row_of(parity, 1)
        own = jnp.concatenate([x_ref[r0, 1 - cc], x_ref[r1, 1 - cc]], 0)
        back = ret[p].reshape(pair_rows, width)
        residual = (own.astype(F32) + back.astype(F32)).astype(BF16).astype(F32)
        mlp_in = layer_norm(residual).astype(BF16)
        update = jnp.zeros_like(residual)
        hidden_size = wup.shape[1]
        piece = 512
        for s in range(hidden_size // piece):
            up = dot(mlp_in, wup[:, s * piece : (s + 1) * piece])
            slope = math.sqrt(2.0 / math.pi)
            bent = jnp.tanh(up * (slope + 0.044715 * slope * (up * up)))
            twice = (up + up * bent).astype(BF16)
            update = update + dot(twice, wdown[s * piece : (s + 1) * piece, :])
        joined = (residual + 0.5 * update).astype(BF16)
        for k, r in enumerate((r0, r1)):
            own_rows = joined[k * rows : (k + 1) * rows]
            tall = jnp.concatenate(
                [own_rows[:, 128 * t : 128 * (t + 1)] for t in range(tiles)], 0
            )
            i = 2 * p + k
            outs[i] = dot(put, tall).astype(BF16).reshape(outs.shape[1:])
            deliver(r, 1 - cc, i).start()
        return carry

    def deliver(r, c, i):
        rim = pl.ds(SH_LAT * r, SH_LAT)
        return pltpu.make_async_copy(
            outs.at[i], out_hbm.at[:, rim, pl.ds(side_pairs * c, side_pairs)], osem.at[i]
        )

    span_of = iota((1, tiles * rows), 1)
    inside = span_of % rows
    place = jnp.where(
        inside < real,
        inside // levels * (tiles * levels) + span_of // rows * levels + inside % levels,
        -1,
    )
    put = jnp.where(iota((slab_rows, tiles * rows), 0) == place, 1.0, 0.0).astype(BF16)

    lax.fori_loop(0, 4, join, 0)

    with jax.named_scope("drain"):
        for d in (0, 1):
            for r in range(4):
                forward(r, d, drain)
        for d in (0, 1):
            for cc in (0, 1):
                for rr in (0, 1):
                    backward(d, cc, rr, finish)
        for p in range(4):
            for k in (0, 1):
                r = row_of(parity_to(p // 2, p % 2), k)
                deliver(r, 1 - p % 2, 2 * p + k).wait()


def hand_over(src, dst, held, in_sem, out_sem):
    takes = [pltpu.make_async_copy(src.at[i], held.at[i], in_sem.at[i]) for i in range(src.shape[0])]
    gives = [pltpu.make_async_copy(held.at[i], dst.at[i], out_sem.at[i]) for i in range(src.shape[0])]
    for take in takes:
        take.start()
    for take, give in zip(takes, gives):
        take.wait()
        give.start()
    for give in gives:
        give.wait()


def per_device(fields, surface_mask, w_qkv, w_out, logit_scale, mask_bias, w_up, w_down):
    groups, levels, nlat, nlon, width = fields.shape
    heads = logit_scale.shape[0]
    head_size = width // heads
    hidden_size = w_up.shape[1]
    tris, sides = nlat // SH_LAT, nlon // SH_LON
    real = groups * levels * SH_LAT * SH_LON
    rows = -(-(real + 1) // 16) * 16
    total = 8 * rows

    tiles = width // 128
    raw = fields.reshape(groups, levels, nlat, nlon, tiles, 128)
    raw = jnp.transpose(raw, (0, 2, 3, 4, 1, 5))
    raw = raw.reshape(groups, nlat, nlon // 2, 2 * tiles * levels, 128)

    vmem = pl.BlockSpec(memory_space=pltpu.VMEM)
    scalars = pl.BlockSpec(memory_space=pltpu.SMEM)
    anywhere = pl.BlockSpec(memory_space=pl.ANY)
    joined = pl.pallas_call(
        functools.partial(kernel, real, heads),
        out_shape=jax.ShapeDtypeStruct(raw.shape, BF16),
        in_specs=[anywhere, vmem, scalars, scalars] + [anywhere] * 4,
        out_specs=anywhere,
        scratch_shapes=[
            pltpu.VMEM(raw.shape, BF16),
            pltpu.VMEM((nlat * levels, 128), F32),
            pltpu.VMEM((tris, sides, rows, width), BF16),
            pltpu.VMEM(w_qkv.shape, BF16),
            pltpu.VMEM(w_out.shape, BF16),
            pltpu.VMEM(w_up.shape, BF16),
            pltpu.VMEM(w_down.shape, BF16),
            pltpu.VMEM((4, 2, rows, width), BF16),
            pltpu.VMEM((4, 2, rows, width), BF16),
            pltpu.VMEM((4, 2, rows, width), BF16),
            pltpu.VMEM((total // 2, width), BF16),
            pltpu.VMEM((heads // 2, total, 2 * head_size), BF16),
            pltpu.VMEM((heads // 2, total, 2 * head_size), BF16),
            pltpu.VMEM((heads // 2, total, 2 * head_size), BF16),
            pltpu.VMEM((total, 2 * head_size), BF16),
            pltpu.VMEM((heads // 2, 2, total // 2, 4 * head_size), F32),
            pltpu.VMEM((8, groups, SH_LAT, SH_LON // 2) + raw.shape[3:], BF16),
            pltpu.SemaphoreType.DMA((5,)),
            pltpu.SemaphoreType.DMA((8,)),
            pltpu.SemaphoreType.DMA((8,)),
            pltpu.SemaphoreType.DMA((8,)),
            pltpu.SemaphoreType.DMA((8,)),
            pltpu.SemaphoreType.DMA((8,)),
        ],
        compiler_params=pltpu.CompilerParams(
            collective_id=0, has_side_effects=True, vmem_limit_bytes=56 * 1024 * 1024
        ),
        name="window_block",
    )(raw, jnp.transpose(surface_mask, (1, 0, 2)), logit_scale, mask_bias, w_qkv, w_out, w_up, w_down)

    joined = pl.pallas_call(
        hand_over,
        out_shape=jax.ShapeDtypeStruct(raw.shape, BF16),
        in_specs=[anywhere],
        out_specs=anywhere,
        scratch_shapes=[
            pltpu.VMEM(raw.shape, BF16),
            pltpu.SemaphoreType.DMA((groups,)),
            pltpu.SemaphoreType.DMA((groups,)),
        ],
        name="hand_over",
    )(joined)
    joined = joined.reshape(groups, nlat, nlon, tiles, levels, 128)
    return jnp.transpose(joined, (0, 4, 1, 2, 3, 5)).reshape(fields.shape)


def solution(mesh):
    return jax.shard_map(
        per_device,
        mesh=mesh,
        in_specs=(
            P("grp", None, "lat", "lon", None),
            P(None, "lat", "lon"),
            P(),
            P(),
            P(),
            P(),
            P(),
            P(),
        ),
        out_specs=P("grp", None, "lat", "lon", None),
        check_vma=False,
    )
```
